32 devices in a mesh: expert: 4 (over y, x), dp: 8 (over z, core).
Axes of the slice: x: 2, y: 2, z: 4, core: 2. Of those that a mesh axis runs over, the one named last changes fastest.
Arguments:
- pool_tokens: bfloat16 [16384, 2048], P('dp', 'expert'), may hold values from -6 to 6
- pool_cotangent: bfloat16 [16384, 2048], P('dp', 'expert'), may hold values from -6 to 6
- token_ids: int32 [4, 4096], P('expert', 'dp'), may hold values from 0 to 2047, as said below
- route_weights: float32 [4, 4096], P('expert', 'dp'), may hold values from 0.1 to 1
- gate_weight: float32 [4, 2048, 512], P('expert', 'dp'), may hold values from -0.125 to 0.125
- up_weight: float32 [4, 2048, 512], P('expert', 'dp'), may hold values from -0.125 to 0.125
- down_weight: float32 [4, 512, 2048], P('expert', 'dp'), may hold values from -0.25 to 0.25
- momentum_gate: float32 [4, 2048, 512], P('expert', 'dp'), may hold values from -0.6 to 0.6
- momentum_up: float32 [4, 2048, 512], P('expert', 'dp'), may hold values from -0.6 to 0.6
- momentum_down: float32 [4, 512, 2048], P('expert', 'dp'), may hold values from -0.6 to 0.6
Outputs:
- new_gate: float32 [4, 2048, 512], P('expert', 'dp')
- new_up: float32 [4, 2048, 512], P('expert', 'dp')
- new_down: float32 [4, 512, 2048], P('expert', 'dp')
- new_momentum_gate: float32 [4, 2048, 512], P('expert', 'dp')
- new_momentum_up: float32 [4, 2048, 512], P('expert', 'dp')
- new_momentum_down: float32 [4, 512, 2048], P('expert', 'dp')
- pool_grad: float32 [16384, 2048], P('dp', 'expert')
The draws below stay inside these ranges and needn't reach their ends.
Inputs may be any that keep to these rules, and one draw needn't show every extreme that they name: `token_ids`: within one expert's 512 slots of one dp index the ids are distinct rows of that index's pool.
All inputs are finite; a program needn't handle non-finite values.
Results may differ from the reference program's by a relative error of at most 0.0066.
Values may be sent and summed in bfloat16 or wider, within the bound.
A program may use at most 128 MiB of HBM per device.

```python
import math
import jax
import jax.numpy as jnp
from jax import lax

D = 2048
H = 512
TOK_DEV = 512
POOL = 2048
EXPERTS = 4
TOKENS = 4096
POOL_ALL = 16384
N_EXPERT = 4
N_DP = 8


def draw_token_ids(key, part):
    subkeys = jax.random.split(key, N_EXPERT * N_DP)
    orders = jax.vmap(lambda single: jax.random.permutation(single, POOL)[:TOK_DEV])(subkeys)
    return orders.reshape(N_EXPERT, N_DP * TOK_DEV).astype(jnp.int32)


def draw_pool_cotangent(key, part):
    column_mean = jax.random.normal(jax.random.fold_in(key, 11), (D,), jnp.float32)
    fluctuation = jax.random.normal(jax.random.fold_in(key, 12), (N_DP * POOL, D), jnp.float32)
    values = column_mean[None, :] + 0.5 * fluctuation
    return jnp.clip(values, -6.0, 6.0).astype(jnp.bfloat16)


def block_levels(rng, extent, shards, smallest, top_value):
    def one(axis_at, shards_of):
        heights = jax.random.uniform(jax.random.fold_in(jax.random.fold_in(rng, 6), axis_at), (shards_of,), jnp.float32, smallest / len(shards), top_value / len(shards))
        return jnp.repeat(jnp.exp(heights), extent[axis_at] // shards_of).reshape((-1,) + (1,) * (len(extent) - axis_at - 1))

    gain = one(*shards[0])
    for cut in shards[1:]:
        gain = gain * one(*cut)
    return gain


def scatter_about(rng, dims, spread, reach, pieces=(), kind=jnp.bfloat16):
    factor_of = block_levels(rng, dims, pieces, -0.22, 0.18) if pieces else 1.0
    array = jax.random.normal(rng, dims, jnp.float32) * spread * factor_of
    return jnp.minimum(jnp.maximum(array, -reach), reach).astype(kind)


def setup_inputs(seed: int = 0) -> dict:
    key_list = jax.random.split(jax.random.key(seed), 11)
    return {
        "pool_tokens": scatter_about(key_list[0], (POOL_ALL, D), 1.0, 6.0, ((0, 8), (1, 4))),
        "pool_cotangent": draw_pool_cotangent(jax.random.fold_in(key_list[10], 71), 0),
        "token_ids": draw_token_ids(jax.random.fold_in(key_list[10], 71), 0),
        "route_weights": jnp.clip(jnp.exp(math.log(1.0) - 2.3025851 * jax.random.uniform(key_list[3], (EXPERTS, TOKENS), jnp.float32) ** block_levels(key_list[3], (EXPERTS, TOKENS), ((0, 4), (1, 8)), -0.2, 0.2)), 0.1, 1.0),
        "gate_weight": scatter_about(key_list[4], (EXPERTS, D, H), D ** -0.5, 0.125, ((0, 4), (1, 8)), jnp.float32),
        "up_weight": scatter_about(key_list[5], (EXPERTS, D, H), D ** -0.5, 0.125, ((0, 4), (1, 8)), jnp.float32),
        "down_weight": scatter_about(key_list[6], (EXPERTS, H, D), H ** -0.5, 0.25, ((0, 4), (1, 8)), jnp.float32),
        "momentum_gate": scatter_about(key_list[7], (EXPERTS, D, H), 0.1, 0.6, ((0, 4), (1, 8)), jnp.float32),
        "momentum_up": scatter_about(key_list[8], (EXPERTS, D, H), 0.1, 0.6, ((0, 4), (1, 8)), jnp.float32),
        "momentum_down": scatter_about(key_list[9], (EXPERTS, H, D), 0.1, 0.6, ((0, 4), (1, 8)), jnp.float32),
    }


momentum_decay = 0.9
learning_rate = 0.05
epsilon = 1e-6


def expert_terms(gate_full, up_full, down_full, pool_x, pool_c, row_ids, route):
    routed = pool_x[row_ids]
    cot_rows = pool_c[row_ids]
    gate_pre = jnp.dot(routed, gate_full, preferred_element_type=jnp.float32)
    up_pre = jnp.dot(routed, up_full, preferred_element_type=jnp.float32)
    sig = jax.nn.sigmoid(gate_pre)
    act = gate_pre * sig
    hidden = (act * up_pre).astype(jnp.bfloat16)
    scaled_cot = (route[:, None] * cot_rows.astype(jnp.float32)).astype(jnp.bfloat16)
    grad_down = lax.dot_general(hidden, scaled_cot, (((0,), (0,)), ((), ())), preferred_element_type=jnp.float32) / TOK_DEV
    hidden_grad = lax.dot_general(scaled_cot, down_full, (((1,), (1,)), ((), ())), preferred_element_type=jnp.float32)
    gate_grad = (hidden_grad * up_pre * sig * (1.0 + gate_pre * (1.0 - sig))).astype(jnp.bfloat16)
    up_grad = (hidden_grad * act).astype(jnp.bfloat16)
    grad_gate = lax.dot_general(routed, gate_grad, (((0,), (0,)), ((), ())), preferred_element_type=jnp.float32) / TOK_DEV
    grad_up = lax.dot_general(routed, up_grad, (((0,), (0,)), ((), ())), preferred_element_type=jnp.float32) / TOK_DEV
    slot_grad = lax.dot_general(gate_grad, gate_full, (((1,), (1,)), ((), ())), preferred_element_type=jnp.float32)
    slot_grad = slot_grad + lax.dot_general(up_grad, up_full, (((1,), (1,)), ((), ())), preferred_element_type=jnp.float32)
    pool_term = jax.ops.segment_sum(slot_grad, row_ids, num_segments=POOL)
    grads = jnp.stack([grad_gate.reshape(-1), grad_up.reshape(-1), grad_down.reshape(-1)])
    return grads, pool_term


def adasum_merge(left_part, right_part):
    inner = jnp.sum(left_part * right_part, axis=-1)
    norm_left = jnp.sum(left_part * left_part, axis=-1)
    norm_right = jnp.sum(right_part * right_part, axis=-1)
    coef_left = 1.0 - inner / (2.0 * (norm_left + epsilon))
    coef_right = 1.0 - inner / (2.0 * (norm_right + epsilon))
    return coef_left[..., None] * left_part + coef_right[..., None] * right_part


def reference(pool_tokens, pool_cotangent, token_ids, route_weights, gate_weight, up_weight, down_weight, momentum_gate, momentum_up, momentum_down):
    pool_x = pool_tokens.reshape(N_DP, POOL, D)
    pool_c = pool_cotangent.reshape(N_DP, POOL, D)
    tiers = N_DP.bit_length() - 1

    def per_expert(running, expert_items):
        ids_e, route_e, gate_e, up_e, down_e, mom_gate, mom_up, mom_down = expert_items
        gate_full = gate_e.astype(jnp.bfloat16)
        up_full = up_e.astype(jnp.bfloat16)
        down_full = down_e.astype(jnp.bfloat16)

        def per_device(device_items):
            return expert_terms(gate_full, up_full, down_full, device_items[0], device_items[1], device_items[2], device_items[3])

        grads, pool_terms = lax.map(per_device, (pool_x, pool_c, ids_e.reshape(N_DP, TOK_DEV), route_e.reshape(N_DP, TOK_DEV)))
        running = running + pool_terms
        merged = grads
        for tier in range(tiers):
            paired = merged.reshape(merged.shape[0] // 2, 2, 3, D * H)
            merged = adasum_merge(paired[:, 0], paired[:, 1])
        merged = merged[0]
        next_gate = momentum_decay * mom_gate + merged[0].reshape(D, H)
        next_up = momentum_decay * mom_up + merged[1].reshape(D, H)
        next_down = momentum_decay * mom_down + merged[2].reshape(H, D)
        return running, (gate_e - learning_rate * next_gate, up_e - learning_rate * next_up, down_e - learning_rate * next_down, next_gate, next_up, next_down)

    start = jnp.zeros((N_DP, POOL, D), jnp.float32)
    running, updated = lax.scan(per_expert, start, (token_ids, route_weights, gate_weight, up_weight, down_weight, momentum_gate, momentum_up, momentum_down))
    return updated[0], updated[1], updated[2], updated[3], updated[4], updated[5], running.reshape(N_DP * POOL, D)
```

```python
import functools

import jax
import jax.numpy as jnp
from jax import lax
from jax.experimental import pallas as pl
from jax.experimental.pallas import tpu as pltpu
from jax.sharding import PartitionSpec as P


momentum_decay = 0.9
learning_rate = 0.05
epsilon = 1e-06
GATE, UP, DOWN = 0, 1, 2


def coefs(inner, norm):
    return 1.0 - inner / (2.0 * (norm + epsilon))


def chunks_of(blocks):
    return min(2, blocks)


def step_kernel(
    n_e, n_dp,
    ids, route, tok_h, cot_h, gate_h, up_h, down_h, mom_gate_h, mom_up_h, mom_down_h,
    new_gate_h, new_up_h, new_down_h, next_gate_h, next_up_h, next_down_h, pool_h,
    tokens, cot, weights, moments, all_ids, stage_x, stage_c, routed, cot_rows,
    gu_full, dn_full, x_t, h_t, hidden, pre, both, slot_grad, returned, pool,
    own, sent, outs, ins, stats, stats_in,
    in_sem, out_sem, id_send, id_recv, tok_send, tok_recv, line_send, line_recv, pair_send, pair_recv,
    ret_send, ret_recv, blk_send, blk_recv, st_send, st_recv,
):
    f32, bf16 = jnp.float32, jnp.bfloat16
    MESH = pl.DeviceIdType.MESH
    me, me_e = lax.axis_index("dp"), lax.axis_index("expert")
    chips = n_dp // 2
    chip, core = me // 2, me % 2
    tiers = n_dp.bit_length() - 1
    half = n_dp // 2
    slots = ids.shape[1]
    pool_rows, width = tokens.shape
    hid = pre.shape[1] // 2
    rows_gu, rows_dn = gate_h.shape[1], down_h.shape[1]
    rows = (rows_gu, rows_gu, rows_dn)
    cols = (hid, hid, down_h.shape[2])
    lump = min(512, hid)
    peers_e = sorted(range(1, n_e), key=lambda d: -bin(d).count("1"))

    barrier = pltpu.get_barrier_semaphore()
    for d in range(1, n_e):
        pl.semaphore_signal(barrier, inc=1, device_id={"expert": me_e ^ d}, device_id_type=MESH)
    for d in range(1, n_dp):
        pl.semaphore_signal(barrier, inc=1, device_id={"dp": me ^ d}, device_id_type=MESH)

    loads = [
        pltpu.make_async_copy(src, dst, in_sem.at[i])
        for i, (src, dst) in enumerate(
            (
                (gate_h.at[0], weights[GATE]), (up_h.at[0], weights[UP]), (down_h.at[0], weights[DOWN]),
                (tok_h, tokens), (cot_h, cot),
                (mom_gate_h.at[0], moments[GATE]), (mom_up_h.at[0], moments[UP]), (mom_down_h.at[0], moments[DOWN]),
            )
        )
    ]
    for copy in loads:
        copy.start()

    def remote(src, dst, ssem, rsem, device):
        return pltpu.make_async_remote_copy(
            src_ref=src, dst_ref=dst, send_sem=ssem, recv_sem=rsem, device_id=device, device_id_type=MESH
        )

    def block(index, size):
        return pl.ds(pl.multiple_of(index * size, size), size)

    def dot(a, b):
        return jnp.dot(a, b, preferred_element_type=f32)

    def dot_t(a, b):
        return lax.dot_general(a, b, (((1,), (1,)), ((), ())), preferred_element_type=f32)

    pending = []

    def send(*args):
        copy = remote(*args)
        copy.start()
        pending.append(copy)
        return copy

    mine_gu, mine_dn = block(me, rows_gu), block(me, rows_dn)
    loads[0].wait()
    gu_full[mine_gu, :hid] = weights[GATE][...].astype(bf16)
    loads[1].wait()
    gu_full[mine_gu, hid:] = weights[UP][...].astype(bf16)
    loads[2].wait()
    dn_full[mine_dn, :] = weights[DOWN][...].astype(bf16)

    pl.semaphore_wait(barrier, n_e + n_dp - 2)

    id_copies = [None] + [
        send(ids, all_ids.at[d], id_send.at[d], id_recv.at[d], {"expert": me_e ^ d}) for d in range(1, n_e)
    ]
    all_ids[0] = ids[...]

    fulls, shard_rows = (gu_full, dn_full), (rows_gu, rows_dn)

    def shard(part, origin):
        return fulls[part].at[block(origin, shard_rows[part])]

    def along(way, hop, part):
        side = 0 if way > 0 else 1
        origin = me - 2 * way * hop
        return remote(
            shard(part, origin), shard(part, origin),
            line_send.at[side, hop, part], line_recv.at[side, hop, part], {"dp": me + 2 * way},
        )

    def arriving(way, hop, part):
        side = 0 if way > 0 else 1
        origin = me - 2 * way * (hop + 1)
        return remote(
            shard(part, origin), shard(part, origin),
            line_send.at[side, hop, part], line_recv.at[side, hop, part], {"dp": me ^ 1},
        )

    def across(way, hop, part):
        side = 0 if way > 0 else 1
        origin = me - 2 * way * hop
        return remote(
            shard(part, origin), shard(part, origin),
            pair_send.at[side, hop, part], pair_recv.at[side, hop, part], {"dp": me ^ 1},
        )

    def across_arriving(way, hop, part):
        side = 0 if way > 0 else 1
        origin = (me ^ 1) - 2 * way * hop
        return remote(
            shard(part, origin), shard(part, origin),
            pair_send.at[side, hop, part], pair_recv.at[side, hop, part], {"dp": me ^ 1},
        )

    def has(way, hop):
        behind = chip >= hop if way > 0 else chip < chips - hop
        ahead = chip < chips - 1 if way > 0 else chip >= 1
        return behind, ahead

    for part in (0, 1):
        for way in (1, -1):
            @pl.when(has(way, 0)[1])
            def _(way=way, part=part):
                along(way, 0, part).start()
    for part in (0, 1):
        across(1, 0, part).start()

    def forward(hop, part):
        for way in (1, -1):
            behind, ahead = has(way, hop + 1)

            @pl.when(behind)
            def _(way=way):
                arriving(way, hop, part).wait_recv()

            @pl.when(jnp.logical_and(behind, ahead))
            def _(way=way):
                along(way, hop + 1, part).start()

            @pl.when(behind)
            def _(way=way):
                across(way, hop + 1, part).start()

    def crossed(hop, part):
        if hop == 0:
            across_arriving(1, 0, part).wait_recv()
            return
        for way in (1, -1):
            @pl.when(has(way, hop)[0])
            def _(way=way):
                across_arriving(way, hop, part).wait_recv()

    lane = lax.broadcasted_iota(jnp.int32, (slots, 128), 1)

    def chosen(d):
        column = jnp.transpose(jnp.broadcast_to(all_ids[d], (128, slots)))
        return jnp.concatenate(
            [jnp.where(column == lane + c * 128, 1.0, 0.0).astype(bf16) for c in range(pool_rows // 128)], axis=1
        )

    own_cols = block(me_e, width)
    loads[3].wait()
    for d in peers_e:
        id_copies[d].wait_recv()
        stage_x[d - 1] = dot(chosen(d), tokens[...]).astype(bf16)
        send(stage_x.at[d - 1], routed.at[:, own_cols], tok_send.at[d, 0], tok_recv.at[d, 0], {"expert": me_e ^ d})
    loads[4].wait()
    for d in peers_e:
        stage_c[d - 1] = dot(chosen(d), cot[...]).astype(bf16)
        send(stage_c.at[d - 1], cot_rows.at[:, own_cols], tok_send.at[d, 1], tok_recv.at[d, 1], {"expert": me_e ^ d})

    last_hop = chips - 1
    forward(0, 0)
    choice = chosen(0)
    routed[:, own_cols] = dot(choice, tokens[...]).astype(bf16)
    cot_rows[:, own_cols] = dot(choice, cot[...]).astype(bf16)
    forward(0, 1)

    route_column = jnp.transpose(jnp.broadcast_to(route[...], (128, slots)))

    def tokens_in(d, part):
        land = (routed, cot_rows)[part]
        theirs = block(me_e ^ d, width)
        stage = (stage_x, stage_c)[part]
        remote(
            stage.at[d - 1], land.at[:, theirs], tok_send.at[d, part], tok_recv.at[d, part], {"expert": me_e ^ d}
        ).wait_recv()

    def turn(d):
        e = me_e ^ d
        per = width // rows_gu
        flipped = jnp.transpose(routed[:, block(e, width)])
        for i in range(per):
            at = block(e * (per // 2) + i // 2, rows_gu)
            x_t[(i % 2) ^ core, at, :] = flipped[i * rows_gu : (i + 1) * rows_gu]

    def scale(d):
        for c in range(width // 128):
            at = pl.ds(pl.multiple_of((me_e ^ d) * width + c * 128, 128), 128)
            cot_rows[:, at] = (route_column * cot_rows[:, at].astype(f32)).astype(bf16)

    tall = min(256, slots)

    def multiply(origin, first):
        at = block(origin, 2 * rows_gu)
        for m in range(slots // tall):
            part = dot(routed[m * tall : (m + 1) * tall, at], gu_full[at, :])
            if first:
                pre[m * tall : (m + 1) * tall, :] = part
            else:
                pre[m * tall : (m + 1) * tall, :] += part

    def multiply_hop(hop):
        crossed(hop, 0)
        for way in (1, -1):
            @pl.when(has(way, hop)[0])
            def _(way=way):
                multiply(chip - way * hop, False)

    turn(0)
    scale(0)
    for d in peers_e:
        tokens_in(d, 0)
        turn(d)
    crossed(0, 0)
    multiply(chip, True)
    for hop in range(1, chips):
        if hop > 1:
            forward(hop - 1, 0)
        multiply_hop(hop)
        if 1 < hop < last_hop:
            forward(hop - 1, 1)

    step = 16

    def activate(i, carry):
        at = pl.ds(pl.multiple_of(i * step, step), step)
        gate_pre, up_pre = pre[at, :hid], pre[at, hid:]
        sig = jax.nn.sigmoid(gate_pre)
        act = gate_pre * sig
        hidden[at, :] = (act * up_pre).astype(bf16)
        pre[at, :hid] = up_pre * sig * (1.0 + gate_pre * (1.0 - sig))
        pre[at, hid:] = act
        return carry

    lax.fori_loop(0, slots // step, activate, 0, unroll=2)
    flipped = jnp.transpose(hidden[...])
    for p in range(n_dp):
        h_t[(p % 2) ^ core, (p // 2) * rows_dn : (p // 2 + 1) * rows_dn, :] = flipped[p * rows_dn : (p + 1) * rows_dn]
    for d in peers_e:
        tokens_in(d, 1)
        scale(d)

    offset = [(2 << t) - 2 - t for t in range(tiers)]
    flying, news, totals = {}, {}, {}

    def blocks_at(t):
        return n_dp >> (t + 1)

    def launch(m, t, k):
        size = blocks_at(t) // chunks_of(blocks_at(t)) * rows[m]
        at = pl.ds(k * size, size)
        src = sent[m] if t == 0 else outs[m][t - 1]
        flying[m, t, k] = send(
            src.at[at], ins[m][t].at[at], blk_send.at[m, t, k], blk_recv.at[m, t, k], {"dp": me ^ (1 << t)}
        )

    def launch_all(m, t):
        for k in range(chunks_of(blocks_at(t))):
            launch(m, t, k)

    def gradient(m, away):
        left = h_t if m == DOWN else x_t
        total = half * rows[m]
        tile = min(256, total)
        parts = chunks_of(half)
        done = 0
        for i in range(total // tile):
            at = pl.ds(i * tile, tile)
            for c in range(0, cols[m], 512):
                if m == DOWN:
                    right = cot_rows[:, c : c + 512]
                else:
                    right = both[:, m * hid + c : m * hid + c + min(512, hid)]
                value = dot(left[1 if away else 0, at, :], right) * (1.0 / slots)
                to = pl.ds(c, value.shape[1])
                if away:
                    sent[m][at, to] = value.astype(bf16)
                else:
                    own[m][at, to] = value
            while away and done < parts and (i + 1) * tile >= (done + 1) * (total // parts):
                launch(m, 0, done)
                done += 1

    def low(t):
        return lax.shift_right_logical(me, 1) & ((1 << t) - 1)

    def bit_of(t):
        return lax.shift_right_logical(me, t) & 1

    def fold(x):
        return x[:8] + x[8:]

    def measure(m, t):
        blocks, steps = blocks_at(t), rows[m] // step
        parts = chunks_of(blocks)
        bit, base = bit_of(t), low(t)
        acc = tuple(jnp.zeros((8, lump), f32) for _ in range(3))

        def body(i, acc):
            j, r = i // steps, i % steps
            at_mine = pl.ds(pl.multiple_of(((j << t) + base) * rows[m] + r * step, step), step)
            at_other = pl.ds(pl.multiple_of(i * step, step), step)
            ab, aa, bb = acc
            for c in range(0, cols[m], lump):
                a = own[m][at_mine, c : c + lump]
                b = ins[m][t][at_other, c : c + lump].astype(f32)
                ab, aa, bb = ab + fold(a * b), aa + fold(a * a), bb + fold(b * b)
            return ab, aa, bb

        per = blocks // parts * steps
        for k in range(parts):
            flying[m, t, k].wait_recv()
            acc = lax.fori_loop(k * per, (k + 1) * per, body, acc, unroll=2 if per % 2 == 0 else 1)

        def lanes(x):
            total = x[:, :128]
            for c in range(1, lump // 128):
                total = total + x[:, c * 128 : (c + 1) * 128]
            return jnp.sum(total, axis=0, keepdims=True)

        ab, aa, bb = (lanes(x) for x in acc)
        local = jnp.concatenate(
            [ab, jnp.where(bit == 0, aa, bb), jnp.where(bit == 0, bb, aa), jnp.zeros((5, 128), f32)], axis=0
        )
        stats[m, t] = local
        totals[m, t] = local
        news[m, t] = [
            send(
                stats.at[m, t], stats_in.at[m, offset[t] + d - 1],
                st_send.at[m, offset[t] + d - 1], st_recv.at[m, offset[t] + d - 1], {"dp": me ^ d},
            )
            for d in range(1, 2 << t)
        ]

    def settle(m, t):
        total = totals[m, t]
        for d in range(1, 2 << t):
            news[m, t][d - 1].wait_recv()
            total = total + stats_in[m, offset[t] + d - 1]
        whole = jnp.sum(total, axis=1, keepdims=True)
        inner, bit = whole[0:1], bit_of(t)
        c_left, c_right = coefs(inner, whole[1:2]), coefs(inner, whole[2:3])
        c_mine = jnp.where(bit == 0, c_left, c_right)
        c_other = jnp.where(bit == 0, c_right, c_left)
        return jnp.broadcast_to(c_mine, (1, lump)), jnp.broadcast_to(c_other, (1, lump))

    def combine(m, t, c_m, c_o, count, which, store):
        steps, base = rows[m] // step, low(t)

        def body(i, carry):
            jj, r = i // steps, i % steps
            j = which(jj)
            at_mine = pl.ds(pl.multiple_of(((j << t) + base) * rows[m] + r * step, step), step)
            at_other = pl.ds(pl.multiple_of(j * rows[m] + r * step, step), step)
            for c in range(0, cols[m], lump):
                value = own[m][at_mine, c : c + lump] * c_m
                value = value + ins[m][t][at_other, c : c + lump].astype(f32) * c_o
                store(i, at_mine, pl.ds(c, lump), value)
            return carry

        n = count * steps
        lax.fori_loop(0, n, body, 0, unroll=2 if n % 2 == 0 else 1)

    def merge(m, t, hold=False):
        c_m, c_o = settle(m, t)
        up = bit_of(t + 1)
        count = blocks_at(t + 1)

        def store_away(i, at, to, value):
            outs[m][t][pl.ds(pl.multiple_of(i * step, step), step), to] = value.astype(bf16)

        def store_own(i, at, to, value):
            own[m][at, to] = value

        combine(m, t, c_m, c_o, count, lambda j: 2 * j + 1 - up, store_away)
        if not hold:
            launch_all(m, t + 1)
        combine(m, t, c_m, c_o, count, lambda j: 2 * j + up, store_own)

    weights_out = (new_gate_h, new_up_h, new_down_h)
    moments_out = (next_gate_h, next_up_h, next_down_h)
    stores = []

    def put(src, dst):
        copy = pltpu.make_async_copy(src, dst, out_sem.at[len(stores)])
        copy.start()
        stores.append(copy)

    def finish(m):
        t = tiers - 1
        c_m, c_o = settle(m, t)
        loads[5 + m].wait()

        def store(i, at, to, value):
            row = pl.ds(pl.multiple_of(i * step, step), step)
            following = momentum_decay * moments[m][row, to] + value
            moments[m][row, to] = following
            weights[m][row, to] = weights[m][row, to] - learning_rate * following

        combine(m, t, c_m, c_o, 1, lambda j: j, store)
        put(moments[m], moments_out[m].at[0])
        put(weights[m], weights_out[m].at[0])

    gradient(DOWN, True)
    gradient(DOWN, False)
    forward(last_hop - 1, 1)
    measure(DOWN, 0)

    for hop in range(chips):
        crossed(hop, 1)
    for m in range(slots // tall):
        at = slice(m * tall, (m + 1) * tall)
        back = dot_t(cot_rows[at, :], dn_full[...])
        both[at, :hid] = (back * pre[at, :hid]).astype(bf16)
        both[at, hid:] = (back * pre[at, hid:]).astype(bf16)
    merge(DOWN, 0)

    def slot_back(d):
        weight = gu_full[block(me_e ^ d, width), :]
        value = dot_t(both[...], weight).astype(bf16)
        if d == 0:
            returned[0:slots, :] = value
            return None
        slot_grad[d - 1] = value
        return send(
            slot_grad.at[d - 1], returned.at[pl.ds(d * slots, slots)], ret_send.at[d], ret_recv.at[d],
            {"expert": me_e ^ d},
        )

    def pool_sum():
        for copy in back_copies:
            copy.wait_recv()
        tile = 256

        @pl.loop(0, pool_rows // tile)
        def _(t):
            at = pl.multiple_of(t * tile, tile)
            row = lax.broadcasted_iota(jnp.int32, (tile, slots), 0) + at
            pick = jnp.concatenate(
                [jnp.where(row == all_ids[d], 1.0, 0.0).astype(bf16) for d in range(n_e)], axis=1
            )
            pool[pl.ds(at, tile), :] = dot(pick, returned[...])

        put(pool, pool_h)

    gradient(GATE, True)
    gradient(UP, True)
    gradient(GATE, False)
    measure(GATE, 0)
    gradient(UP, False)
    merge(GATE, 0)
    measure(UP, 0)
    back_copies = [slot_back(d) for d in peers_e]
    merge(UP, 0, hold=True)
    order = sorted(
        ((m, t) for m in range(3) for t in range(1, tiers)), key=lambda x: (2 * (x[1] - 1) + (x[0] + 1) % 3, -x[1])
    )
    for m, t in order:
        measure(m, t)
        if (m, t) == (DOWN, 1):
            slot_back(0)
        if t == tiers - 1:
            finish(m)
        else:
            merge(m, t)
        if (m, t) == (DOWN, 1):
            launch_all(UP, 1)
        if (m, t) == (DOWN, 2):
            pool_sum()

    for part in (0, 1):
        across(1, 0, part).wait_send()
    for hop in range(chips):
        for part in (0, 1):
            for way in (1, -1):
                behind, ahead = has(way, hop)

                @pl.when(jnp.logical_and(behind, ahead))
                def _(way=way, hop=hop, part=part):
                    along(way, hop, part).wait_send()

                if hop:
                    @pl.when(behind)
                    def _(way=way, hop=hop, part=part):
                        across(way, hop, part).wait_send()
    for copy in pending:
        copy.wait_send()
    for copy in stores:
        copy.wait()


def local(
    pool_tokens,
    pool_cotangent,
    token_ids,
    route_weights,
    gate_weight,
    up_weight,
    down_weight,
    momentum_gate,
    momentum_up,
    momentum_down,
):
    bf16, f32 = jnp.bfloat16, jnp.float32
    n_e, n_dp = lax.axis_size("expert"), lax.axis_size("dp")
    chips, half, tiers = n_dp // 2, n_dp // 2, n_dp.bit_length() - 1
    pool_rows, width = pool_tokens.shape
    slots = token_ids.shape[1]
    rows_gu, hid = gate_weight.shape[1:]
    rows_dn, full = down_weight.shape[1:]
    shapes = ((rows_gu, hid), (rows_gu, hid), (rows_dn, full))
    n_stats = sum((2 << t) - 1 for t in range(tiers))
    vmem, anywhere = pl.BlockSpec(memory_space=pltpu.VMEM), pl.BlockSpec(memory_space=pl.ANY)
    dma, buf = pltpu.SemaphoreType.DMA, pltpu.VMEM

    def per_matrix(blocks, kind):
        return [buf((blocks * r, c), kind) for r, c in shapes]

    def per_tier(first, kind):
        return [[buf(((n_dp >> (t + 1)) * r, c), kind) for t in range(first, tiers)] for r, c in shapes]

    like = [jax.ShapeDtypeStruct(x.shape, f32) for x in (gate_weight, up_weight, down_weight)]
    return pl.pallas_call(
        functools.partial(step_kernel, n_e, n_dp),
        out_shape=(*like, *like, jax.ShapeDtypeStruct((pool_rows, width), f32)),
        in_specs=[vmem] * 2 + [anywhere] * 8,
        out_specs=(anywhere,) * 7,
        scratch_shapes=[
            buf((pool_rows, width), bf16),
            buf((pool_rows, width), bf16),
            per_matrix(1, f32),
            per_matrix(1, f32),
            buf((n_e, 1, slots), jnp.int32),
            buf((n_e - 1, slots, width), bf16),
            buf((n_e - 1, slots, width), bf16),
            buf((slots, full), bf16),
            buf((slots, full), bf16),
            buf((n_dp * rows_gu, 2 * hid), bf16),
            buf((n_dp * rows_dn, full), bf16),
            buf((2, half * rows_gu, slots), bf16),
            buf((2, half * rows_dn, slots), bf16),
            buf((slots, hid), bf16),
            buf((slots, 2 * hid), f32),
            buf((slots, 2 * hid), bf16),
            buf((n_e - 1, slots, width), bf16),
            buf((n_e * slots, width), bf16),
            buf((pool_rows, width), f32),
            per_matrix(half, f32),
            per_matrix(half, bf16),
            per_tier(1, bf16),
            per_tier(0, bf16),
            buf((3, tiers, 8, 128), f32),
            buf((3, n_stats, 8, 128), f32),
            dma((8,)), dma((7,)), dma((n_e,)), dma((n_e,)), dma((n_e, 2)), dma((n_e, 2)),
            dma((2, chips, 2)), dma((2, chips, 2)), dma((2, chips, 2)), dma((2, chips, 2)),
            dma((n_e,)), dma((n_e,)), dma((3, tiers, 2)), dma((3, tiers, 2)), dma((3, n_stats)), dma((3, n_stats)),
        ],
        compiler_params=pltpu.CompilerParams(
            collective_id=1, has_side_effects=True, vmem_limit_bytes=63 * 1024 * 1024
        ),
    )(
        token_ids, route_weights, pool_tokens, pool_cotangent, gate_weight, up_weight, down_weight,
        momentum_gate, momentum_up, momentum_down,
    )


def solution(mesh):
    in_specs = (
        P("dp", "expert"),
        P("dp", "expert"),
        P("expert", "dp"),
        P("expert", "dp"),
        P("expert", "dp", None),
        P("expert", "dp", None),
        P("expert", "dp", None),
        P("expert", "dp", None),
        P("expert", "dp", None),
        P("expert", "dp", None),
    )
    out_specs = (
        P("expert", "dp", None),
        P("expert", "dp", None),
        P("expert", "dp", None),
        P("expert", "dp", None),
        P("expert", "dp", None),
        P("expert", "dp", None),
        P("dp", "expert"),
    )
    return jax.shard_map(local, mesh=mesh, in_specs=in_specs, out_specs=out_specs, check_vma=False)
```

```python
import functools

import jax
import jax.numpy as jnp
from jax import lax
from jax.experimental import pallas as pl
from jax.experimental.pallas import tpu as pltpu
from jax.sharding import PartitionSpec as P


momentum_decay = 0.9
learning_rate = 0.05
epsilon = 1e-06
GATE, UP, DOWN = 0, 1, 2


def coefs(inner, norm):
    return 1.0 - inner / (2.0 * (norm + epsilon))


def chunks_of(blocks):
    return min(2, blocks)


def step_kernel(
    n_e, n_dp,
    ids, route, tok_h, cot_h, gate_h, up_h, down_h, mom_gate_h, mom_up_h, mom_down_h,
    new_gate, new_up, new_down, next_gate, next_up, next_down, pool,
    tokens, cot, weights, moments, all_ids, stage_x, stage_c, routed, cot_rows,
    gu_full, dn_full, x_t, h_t, hidden, pre, both, slot_grad, returned,
    own, sent, outs, ins, stats, stats_in,
    in_sem, id_send, id_recv, tok_send, tok_recv, line_send, line_recv, pair_send, pair_recv,
    ret_send, ret_recv, blk_send, blk_recv, st_send, st_recv,
):
    f32, bf16 = jnp.float32, jnp.bfloat16
    MESH = pl.DeviceIdType.MESH
    me, me_e = lax.axis_index("dp"), lax.axis_index("expert")
    chips = n_dp // 2
    chip, core = me // 2, me % 2
    tiers = n_dp.bit_length() - 1
    half = n_dp // 2
    slots = ids.shape[1]
    pool_rows, width = tokens.shape
    hid = pre.shape[1] // 2
    rows_gu, rows_dn = gate_h.shape[1], down_h.shape[1]
    rows = (rows_gu, rows_gu, rows_dn)
    cols = (hid, hid, down_h.shape[2])
    lump = min(512, hid)
    peers_e = sorted(range(1, n_e), key=lambda d: -bin(d).count("1"))

    barrier = pltpu.get_barrier_semaphore()
    for d in range(1, n_e):
        pl.semaphore_signal(barrier, inc=1, device_id={"expert": me_e ^ d}, device_id_type=MESH)
    for d in range(1, n_dp):
        pl.semaphore_signal(barrier, inc=1, device_id={"dp": me ^ d}, device_id_type=MESH)

    loads = [
        pltpu.make_async_copy(src, dst, in_sem.at[i])
        for i, (src, dst) in enumerate(
            (
                (gate_h.at[0], weights[GATE]), (up_h.at[0], weights[UP]), (down_h.at[0], weights[DOWN]),
                (tok_h, tokens), (cot_h, cot),
                (mom_gate_h.at[0], moments[GATE]), (mom_up_h.at[0], moments[UP]), (mom_down_h.at[0], moments[DOWN]),
            )
        )
    ]
    for copy in loads:
        copy.start()

    def remote(src, dst, ssem, rsem, device):
        return pltpu.make_async_remote_copy(
            src_ref=src, dst_ref=dst, send_sem=ssem, recv_sem=rsem, device_id=device, device_id_type=MESH
        )

    def block(index, size):
        return pl.ds(pl.multiple_of(index * size, size), size)

    def dot(a, b):
        return jnp.dot(a, b, preferred_element_type=f32)

    def dot_t(a, b):
        return lax.dot_general(a, b, (((1,), (1,)), ((), ())), preferred_element_type=f32)

    pending = []

    def send(*args):
        copy = remote(*args)
        copy.start()
        pending.append(copy)
        return copy

    mine_gu, mine_dn = block(me, rows_gu), block(me, rows_dn)
    loads[0].wait()
    gu_full[mine_gu, :hid] = weights[GATE][...].astype(bf16)
    loads[1].wait()
    gu_full[mine_gu, hid:] = weights[UP][...].astype(bf16)
    loads[2].wait()
    dn_full[mine_dn, :] = weights[DOWN][...].astype(bf16)

    pl.semaphore_wait(barrier, n_e + n_dp - 2)

    id_copies = [None] + [
        send(ids, all_ids.at[d], id_send.at[d], id_recv.at[d], {"expert": me_e ^ d}) for d in range(1, n_e)
    ]
    all_ids[0] = ids[...]

    fulls, shard_rows = (gu_full, dn_full), (rows_gu, rows_dn)

    def shard(part, origin):
        return fulls[part].at[block(origin, shard_rows[part])]

    def along(way, hop, part):
        side = 0 if way > 0 else 1
        origin = me - 2 * way * hop
        return remote(
            shard(part, origin), shard(part, origin),
            line_send.at[side, hop, part], line_recv.at[side, hop, part], {"dp": me + 2 * way},
        )

    def arriving(way, hop, part):
        side = 0 if way > 0 else 1
        origin = me - 2 * way * (hop + 1)
        return remote(
            shard(part, origin), shard(part, origin),
            line_send.at[side, hop, part], line_recv.at[side, hop, part], {"dp": me ^ 1},
        )

    def across(way, hop, part):
        side = 0 if way > 0 else 1
        origin = me - 2 * way * hop
        return remote(
            shard(part, origin), shard(part, origin),
            pair_send.at[side, hop, part], pair_recv.at[side, hop, part], {"dp": me ^ 1},
        )

    def across_arriving(way, hop, part):
        side = 0 if way > 0 else 1
        origin = (me ^ 1) - 2 * way * hop
        return remote(
            shard(part, origin), shard(part, origin),
            pair_send.at[side, hop, part], pair_recv.at[side, hop, part], {"dp": me ^ 1},
        )

    def has(way, hop):
        behind = chip >= hop if way > 0 else chip < chips - hop
        ahead = chip < chips - 1 if way > 0 else chip >= 1
        return behind, ahead

    for part in (0, 1):
        for way in (1, -1):
            @pl.when(has(way, 0)[1])
            def _(way=way, part=part):
                along(way, 0, part).start()
    for part in (0, 1):
        across(1, 0, part).start()

    def forward(hop, part):
        for way in (1, -1):
            behind, ahead = has(way, hop + 1)

            @pl.when(behind)
            def _(way=way):
                arriving(way, hop, part).wait_recv()

            @pl.when(jnp.logical_and(behind, ahead))
            def _(way=way):
                along(way, hop + 1, part).start()

            @pl.when(behind)
            def _(way=way):
                across(way, hop + 1, part).start()

    def crossed(hop, part):
        if hop == 0:
            across_arriving(1, 0, part).wait_recv()
            return
        for way in (1, -1):
            @pl.when(has(way, hop)[0])
            def _(way=way):
                across_arriving(way, hop, part).wait_recv()

    lane = lax.broadcasted_iota(jnp.int32, (slots, 128), 1)

    def chosen(d):
        column = jnp.transpose(jnp.broadcast_to(all_ids[d], (128, slots)))
        return jnp.concatenate(
            [jnp.where(column == lane + c * 128, 1.0, 0.0).astype(bf16) for c in range(pool_rows // 128)], axis=1
        )

    own_cols = block(me_e, width)
    loads[3].wait()
    for d in peers_e:
        id_copies[d].wait_recv()
        stage_x[d - 1] = dot(chosen(d), tokens[...]).astype(bf16)
        send(stage_x.at[d - 1], routed.at[:, own_cols], tok_send.at[d, 0], tok_recv.at[d, 0], {"expert": me_e ^ d})
    loads[4].wait()
    for d in peers_e:
        stage_c[d - 1] = dot(chosen(d), cot[...]).astype(bf16)
        send(stage_c.at[d - 1], cot_rows.at[:, own_cols], tok_send.at[d, 1], tok_recv.at[d, 1], {"expert": me_e ^ d})

    last_hop = chips - 1
    forward(0, 0)
    choice = chosen(0)
    routed[:, own_cols] = dot(choice, tokens[...]).astype(bf16)
    cot_rows[:, own_cols] = dot(choice, cot[...]).astype(bf16)
    forward(0, 1)

    route_column = jnp.transpose(jnp.broadcast_to(route[...], (128, slots)))

    def tokens_in(d, part):
        land = (routed, cot_rows)[part]
        theirs = block(me_e ^ d, width)
        stage = (stage_x, stage_c)[part]
        remote(
            stage.at[d - 1], land.at[:, theirs], tok_send.at[d, part], tok_recv.at[d, part], {"expert": me_e ^ d}
        ).wait_recv()

    def turn(d):
        e = me_e ^ d
        per = width // rows_gu
        flipped = jnp.transpose(routed[:, block(e, width)])
        for i in range(per):
            at = block(e * (per // 2) + i // 2, rows_gu)
            x_t[(i % 2) ^ core, at, :] = flipped[i * rows_gu : (i + 1) * rows_gu]

    def scale(d):
        for c in range(width // 128):
            at = pl.ds(pl.multiple_of((me_e ^ d) * width + c * 128, 128), 128)
            cot_rows[:, at] = (route_column * cot_rows[:, at].astype(f32)).astype(bf16)

    tall = min(256, slots)

    def multiply(origin, first):
        at = block(origin, 2 * rows_gu)
        for m in range(slots // tall):
            part = dot(routed[m * tall : (m + 1) * tall, at], gu_full[at, :])
            if first:
                pre[m * tall : (m + 1) * tall, :] = part
            else:
                pre[m * tall : (m + 1) * tall, :] += part

    def multiply_hop(hop):
        crossed(hop, 0)
        for way in (1, -1):
            @pl.when(has(way, hop)[0])
            def _(way=way):
                multiply(chip - way * hop, False)

    turn(0)
    scale(0)
    for d in peers_e:
        tokens_in(d, 0)
        turn(d)
    crossed(0, 0)
    multiply(chip, True)
    for hop in range(1, chips):
        if hop > 1:
            forward(hop - 1, 0)
        multiply_hop(hop)
        if 1 < hop < last_hop:
            forward(hop - 1, 1)

    step = 16

    def activate(i, carry):
        at = pl.ds(pl.multiple_of(i * step, step), step)
        gate_pre, up_pre = pre[at, :hid], pre[at, hid:]
        sig = jax.nn.sigmoid(gate_pre)
        act = gate_pre * sig
        hidden[at, :] = (act * up_pre).astype(bf16)
        pre[at, :hid] = up_pre * sig * (1.0 + gate_pre * (1.0 - sig))
        pre[at, hid:] = act
        return carry

    lax.fori_loop(0, slots // step, activate, 0, unroll=2)
    flipped = jnp.transpose(hidden[...])
    for p in range(n_dp):
        h_t[(p % 2) ^ core, (p // 2) * rows_dn : (p // 2 + 1) * rows_dn, :] = flipped[p * rows_dn : (p + 1) * rows_dn]
    for d in peers_e:
        tokens_in(d, 1)
        scale(d)

    offset = [(2 << t) - 2 - t for t in range(tiers)]
    flying, news, totals = {}, {}, {}

    def blocks_at(t):
        return n_dp >> (t + 1)

    def block_copy(m, t, k):
        size = blocks_at(t) // chunks_of(blocks_at(t)) * rows[m]
        at = pl.ds(k * size, size)
        src = sent[m] if t == 0 else outs[m][t - 1]
        return remote(
            src.at[at], ins[m][t].at[at], blk_send.at[m, t, k], blk_recv.at[m, t, k], {"dp": me ^ (1 << t)}
        )

    def launch_all(m, t, now=None):
        for k in range(chunks_of(blocks_at(t))):
            copy = block_copy(m, t, k)
            if now is None:
                copy.start()
            else:
                pl.when(now)(copy.start)
            if (m, t, k) not in flying:
                flying[m, t, k] = copy
                pending.append(copy)

    def gradient(m, away):
        left = h_t if m == DOWN else x_t
        total = half * rows[m]
        tile = min(256, total)
        parts = chunks_of(half)
        done = 0
        for i in range(total // tile):
            at = pl.ds(i * tile, tile)
            for c in range(0, cols[m], 512):
                if m == DOWN:
                    right = cot_rows[:, c : c + 512]
                else:
                    right = both[:, m * hid + c : m * hid + c + min(512, hid)]
                value = dot(left[1 if away else 0, at, :], right) * (1.0 / slots)
                to = pl.ds(c, value.shape[1])
                if away:
                    sent[m][at, to] = value.astype(bf16)
                else:
                    own[m][at, to] = value
            while away and done < parts and (i + 1) * tile >= (done + 1) * (total // parts):
                flying[m, 0, done] = block_copy(m, 0, done)
                flying[m, 0, done].start()
                pending.append(flying[m, 0, done])
                done += 1

    def low(t):
        return lax.shift_right_logical(me, 1) & ((1 << t) - 1)

    def bit_of(t):
        return lax.shift_right_logical(me, t) & 1

    def fold(x):
        return x[:8] + x[8:]

    def measure(m, t):
        blocks, steps = blocks_at(t), rows[m] // step
        parts = chunks_of(blocks)
        bit, base = bit_of(t), low(t)
        acc = tuple(jnp.zeros((8, lump), f32) for _ in range(3))

        def body(i, acc):
            j, r = i // steps, i % steps
            at_mine = pl.ds(pl.multiple_of(((j << t) + base) * rows[m] + r * step, step), step)
            at_other = pl.ds(pl.multiple_of(i * step, step), step)
            ab, aa, bb = acc
            for c in range(0, cols[m], lump):
                a = own[m][at_mine, c : c + lump]
                b = ins[m][t][at_other, c : c + lump].astype(f32)
                ab, aa, bb = ab + fold(a * b), aa + fold(a * a), bb + fold(b * b)
            return ab, aa, bb

        per = blocks // parts * steps
        for k in range(parts):
            flying[m, t, k].wait_recv()
            acc = lax.fori_loop(k * per, (k + 1) * per, body, acc, unroll=2 if per % 2 == 0 else 1)

        def lanes(x):
            total = x[:, :128]
            for c in range(1, lump // 128):
                total = total + x[:, c * 128 : (c + 1) * 128]
            return jnp.sum(total, axis=0, keepdims=True)

        ab, aa, bb = (lanes(x) for x in acc)
        local = jnp.concatenate(
            [ab, jnp.where(bit == 0, aa, bb), jnp.where(bit == 0, bb, aa), jnp.zeros((5, 128), f32)], axis=0
        )
        stats[m, t] = local
        totals[m, t] = local
        news[m, t] = [
            send(
                stats.at[m, t], stats_in.at[m, offset[t] + d - 1],
                st_send.at[m, offset[t] + d - 1], st_recv.at[m, offset[t] + d - 1], {"dp": me ^ d},
            )
            for d in range(1, 2 << t)
        ]

    def settle(m, t):
        total = totals[m, t]
        for d in range(1, 2 << t):
            news[m, t][d - 1].wait_recv()
            total = total + stats_in[m, offset[t] + d - 1]
        whole = jnp.sum(total, axis=1, keepdims=True)
        inner, bit = whole[0:1], bit_of(t)
        c_left, c_right = coefs(inner, whole[1:2]), coefs(inner, whole[2:3])
        c_mine = jnp.where(bit == 0, c_left, c_right)
        c_other = jnp.where(bit == 0, c_right, c_left)
        return jnp.broadcast_to(c_mine, (1, lump)), jnp.broadcast_to(c_other, (1, lump))

    def combine(m, t, c_m, c_o, count, which, store):
        steps, base = rows[m] // step, low(t)

        def body(i, carry):
            jj, r = i // steps, i % steps
            j = which(jj)
            at_mine = pl.ds(pl.multiple_of(((j << t) + base) * rows[m] + r * step, step), step)
            at_other = pl.ds(pl.multiple_of(j * rows[m] + r * step, step), step)
            for c in range(0, cols[m], lump):
                value = own[m][at_mine, c : c + lump] * c_m
                value = value + ins[m][t][at_other, c : c + lump].astype(f32) * c_o
                store(i, at_mine, pl.ds(c, lump), value)
            return carry

        n = count * steps
        lax.fori_loop(0, n, body, 0, unroll=2 if n % 2 == 0 else 1)

    def merge(m, t):
        c_m, c_o = settle(m, t)
        up = bit_of(t + 1)
        count = blocks_at(t + 1)

        def store_away(i, at, to, value):
            outs[m][t][pl.ds(pl.multiple_of(i * step, step), step), to] = value.astype(bf16)

        def store_own(i, at, to, value):
            own[m][at, to] = value

        combine(m, t, c_m, c_o, count, lambda j: 2 * j + 1 - up, store_away)
        combine(m, t, c_m, c_o, count, lambda j: 2 * j + up, store_own)

    new, following = (new_gate, new_up, new_down), (next_gate, next_up, next_down)

    def finish(m):
        t = tiers - 1
        c_m, c_o = settle(m, t)
        loads[5 + m].wait()

        def store(i, at, to, value):
            row = pl.ds(pl.multiple_of(i * step, step), step)
            momentum = momentum_decay * moments[m][row, to] + value
            following[m][0, row, to] = momentum
            new[m][0, row, to] = weights[m][row, to] - learning_rate * momentum

        combine(m, t, c_m, c_o, 1, lambda j: j, store)

    gradient(DOWN, True)
    gradient(DOWN, False)
    forward(last_hop - 1, 1)
    measure(DOWN, 0)

    for hop in range(chips):
        crossed(hop, 1)
    for m in range(slots // tall):
        at = slice(m * tall, (m + 1) * tall)
        back = dot_t(cot_rows[at, :], dn_full[...])
        both[at, :hid] = (back * pre[at, :hid]).astype(bf16)
        both[at, hid:] = (back * pre[at, hid:]).astype(bf16)
    merge(DOWN, 0)

    def slot_back(d):
        weight = gu_full[block(me_e ^ d, width), :]
        value = dot_t(both[...], weight).astype(bf16)
        if d == 0:
            returned[0:slots, :] = value
            return None
        slot_grad[d - 1] = value
        return send(
            slot_grad.at[d - 1], returned.at[pl.ds(d * slots, slots)], ret_send.at[d], ret_recv.at[d],
            {"expert": me_e ^ d},
        )

    def pool_sum():
        for copy in back_copies:
            copy.wait_recv()
        tile = 256

        @pl.loop(0, pool_rows // tile)
        def _(t):
            at = pl.multiple_of(t * tile, tile)
            row = lax.broadcasted_iota(jnp.int32, (tile, slots), 0) + at
            pick = jnp.concatenate(
                [jnp.where(row == all_ids[d], 1.0, 0.0).astype(bf16) for d in range(n_e)], axis=1
            )
            pool[pl.ds(at, tile), :] = dot(pick, returned[...])

    launch_all(DOWN, 1)
    gradient(GATE, True)
    gradient(UP, True)
    gradient(GATE, False)
    measure(GATE, 0)
    gradient(UP, False)
    merge(GATE, 0)
    measure(UP, 0)
    back_copies = [slot_back(d) for d in peers_e]
    merge(UP, 0)
    same_way = bit_of(1) == bit_of(2)
    measure(DOWN, 1)
    launch_all(GATE, 1)
    slot_back(0)
    merge(DOWN, 1)
    launch_all(DOWN, 2, jnp.logical_not(same_way))
    measure(GATE, 1)
    launch_all(DOWN, 2, same_way)
    launch_all(UP, 1)
    merge(GATE, 1)
    launch_all(GATE, 2, jnp.logical_not(same_way))
    pool_sum()
    measure(UP, 1)
    launch_all(GATE, 2, same_way)
    merge(UP, 1)
    launch_all(UP, 2)
    for t in range(2, tiers):
        for m in (DOWN, GATE, UP):
            measure(m, t)
            if t == tiers - 1:
                finish(m)
            else:
                merge(m, t)
                launch_all(m, t + 1)

    for part in (0, 1):
        across(1, 0, part).wait_send()
    for hop in range(chips):
        for part in (0, 1):
            for way in (1, -1):
                behind, ahead = has(way, hop)

                @pl.when(jnp.logical_and(behind, ahead))
                def _(way=way, hop=hop, part=part):
                    along(way, hop, part).wait_send()

                if hop:
                    @pl.when(behind)
                    def _(way=way, hop=hop, part=part):
                        across(way, hop, part).wait_send()
    for copy in pending:
        copy.wait_send()


def store_kernel(*refs):
    *pairs, sem = refs
    count = len(pairs) // 2
    copies = [pltpu.make_async_copy(pairs[i], pairs[count + i], sem.at[i]) for i in range(count)]
    for copy in copies:
        copy.start()
    for copy in copies:
        copy.wait()


def local(
    pool_tokens,
    pool_cotangent,
    token_ids,
    route_weights,
    gate_weight,
    up_weight,
    down_weight,
    momentum_gate,
    momentum_up,
    momentum_down,
):
    bf16, f32 = jnp.bfloat16, jnp.float32
    n_e, n_dp = lax.axis_size("expert"), lax.axis_size("dp")
    chips, half, tiers = n_dp // 2, n_dp // 2, n_dp.bit_length() - 1
    pool_rows, width = pool_tokens.shape
    slots = token_ids.shape[1]
    rows_gu, hid = gate_weight.shape[1:]
    rows_dn, full = down_weight.shape[1:]
    shapes = ((rows_gu, hid), (rows_gu, hid), (rows_dn, full))
    n_stats = sum((2 << t) - 1 for t in range(tiers))
    vmem, anywhere = pl.BlockSpec(memory_space=pltpu.VMEM), pl.BlockSpec(memory_space=pl.ANY)
    dma, buf = pltpu.SemaphoreType.DMA, pltpu.VMEM

    def per_matrix(blocks, kind):
        return [buf((blocks * r, c), kind) for r, c in shapes]

    def per_tier(first, kind):
        return [[buf(((n_dp >> (t + 1)) * r, c), kind) for t in range(first, tiers)] for r, c in shapes]

    like = [(x.shape, f32) for x in (gate_weight, up_weight, down_weight)]
    like = [*like, *like, ((pool_rows, width), f32)]
    results = pl.pallas_call(
        functools.partial(step_kernel, n_e, n_dp),
        out_shape=[buf(*x) for x in like],
        in_specs=[vmem] * 2 + [anywhere] * 8,
        out_specs=[vmem] * len(like),
        scratch_shapes=[
            buf((pool_rows, width), bf16),
            buf((pool_rows, width), bf16),
            per_matrix(1, f32),
            per_matrix(1, f32),
            buf((n_e, 1, slots), jnp.int32),
            buf((n_e - 1, slots, width), bf16),
            buf((n_e - 1, slots, width), bf16),
            buf((slots, full), bf16),
            buf((slots, full), bf16),
            buf((n_dp * rows_gu, 2 * hid), bf16),
            buf((n_dp * rows_dn, full), bf16),
            buf((2, half * rows_gu, slots), bf16),
            buf((2, half * rows_dn, slots), bf16),
            buf((slots, hid), bf16),
            buf((slots, 2 * hid), f32),
            buf((slots, 2 * hid), bf16),
            buf((n_e - 1, slots, width), bf16),
            buf((n_e * slots, width), bf16),
            per_matrix(half, f32),
            per_matrix(half, bf16),
            per_tier(1, bf16),
            per_tier(0, bf16),
            buf((3, tiers, 8, 128), f32),
            buf((3, n_stats, 8, 128), f32),
            dma((8,)), dma((n_e,)), dma((n_e,)), dma((n_e, 2)), dma((n_e, 2)),
            dma((2, chips, 2)), dma((2, chips, 2)), dma((2, chips, 2)), dma((2, chips, 2)),
            dma((n_e,)), dma((n_e,)), dma((3, tiers, 2)), dma((3, tiers, 2)), dma((3, n_stats)), dma((3, n_stats)),
        ],
        compiler_params=pltpu.CompilerParams(
            collective_id=1, has_side_effects=True, vmem_limit_bytes=54 * 1024 * 1024
        ),
    )(
        token_ids, route_weights, pool_tokens, pool_cotangent, gate_weight, up_weight, down_weight,
        momentum_gate, momentum_up, momentum_down,
    )
    return pl.pallas_call(
        store_kernel,
        out_shape=[jax.ShapeDtypeStruct(*x) for x in like],
        in_specs=[vmem] * len(like),
        out_specs=[anywhere] * len(like),
        scratch_shapes=[dma((len(like),))],
        compiler_params=pltpu.CompilerParams(vmem_limit_bytes=1024 * 1024),
    )(*results)


def solution(mesh):
    in_specs = (
        P("dp", "expert"),
        P("dp", "expert"),
        P("expert", "dp"),
        P("expert", "dp"),
        P("expert", "dp", None),
        P("expert", "dp", None),
        P("expert", "dp", None),
        P("expert", "dp", None),
        P("expert", "dp", None),
        P("expert", "dp", None),
    )
    out_specs = (
        P("expert", "dp", None),
        P("expert", "dp", None),
        P("expert", "dp", None),
        P("expert", "dp", None),
        P("expert", "dp", None),
        P("expert", "dp", None),
        P("dp", "expert"),
    )
    return jax.shard_map(local, mesh=mesh, in_specs=in_specs, out_specs=out_specs, check_vma=False)
```

```python
import functools

import jax
import jax.numpy as jnp
from jax import lax
from jax.experimental import pallas as pl
from jax.experimental.pallas import tpu as pltpu
from jax.sharding import PartitionSpec as P


momentum_decay = 0.9
learning_rate = 0.05
epsilon = 1e-06
GATE, UP, DOWN = 0, 1, 2


def coefs(inner, norm):
    return 1.0 - inner / (2.0 * (norm + epsilon))


def chunks_of(blocks):
    return min(2, blocks)


def step_kernel(
    n_e, n_dp,
    ids, route, tok_h, cot_h, gate_h, up_h, down_h, mom_gate_h, mom_up_h, mom_down_h,
    new_gate, new_up, new_down, next_gate, next_up, next_down, pool,
    tokens, cot, weights, moments, all_ids, stage_x, stage_c, routed, cot_rows,
    gu_full, dn_full, x_t, h_t, hidden, pre, both, slot_grad, returned,
    own, sent, outs, ins, stats, stats_in, far_out, far_in, far_stats, far_stats_in,
    in_sem, id_send, id_recv, tok_send, tok_recv, line_send, line_recv, pair_send, pair_recv,
    ret_send, ret_recv, blk_send, blk_recv, st_send, st_recv, dn_send, dn_recv,
    far_send, far_recv, table_send, table_recv,
):
    f32, bf16 = jnp.float32, jnp.bfloat16
    MESH = pl.DeviceIdType.MESH
    me, me_e = lax.axis_index("dp"), lax.axis_index("expert")
    chips = n_dp // 2
    chip, core = me // 2, me % 2
    tiers = n_dp.bit_length() - 1
    half = n_dp // 2
    slots = ids.shape[1]
    pool_rows, width = tokens.shape
    hid = pre.shape[1] // 2
    rows_gu, rows_dn = gate_h.shape[1], down_h.shape[1]
    rows = (rows_gu, rows_gu, rows_dn)
    cols = (hid, hid, down_h.shape[2])
    lump = min(512, hid)
    peers_e = sorted(range(1, n_e), key=lambda d: -bin(d).count("1"))

    barrier = pltpu.get_barrier_semaphore()
    for d in range(1, n_e):
        pl.semaphore_signal(barrier, inc=1, device_id={"expert": me_e ^ d}, device_id_type=MESH)
    for d in range(1, n_dp):
        pl.semaphore_signal(barrier, inc=1, device_id={"dp": me ^ d}, device_id_type=MESH)

    loads = [
        pltpu.make_async_copy(src, dst, in_sem.at[i])
        for i, (src, dst) in enumerate(
            (
                (gate_h.at[0], weights[GATE]), (up_h.at[0], weights[UP]), (down_h.at[0], weights[DOWN]),
                (tok_h, tokens), (cot_h, cot),
                (mom_gate_h.at[0], moments[GATE]), (mom_up_h.at[0], moments[UP]), (mom_down_h.at[0], moments[DOWN]),
            )
        )
    ]
    for copy in loads:
        copy.start()

    def remote(src, dst, ssem, rsem, device):
        return pltpu.make_async_remote_copy(
            src_ref=src, dst_ref=dst, send_sem=ssem, recv_sem=rsem, device_id=device, device_id_type=MESH
        )

    def block(index, size):
        return pl.ds(pl.multiple_of(index * size, size), size)

    def dot(a, b):
        return jnp.dot(a, b, preferred_element_type=f32)

    def dot_t(a, b):
        return lax.dot_general(a, b, (((1,), (1,)), ((), ())), preferred_element_type=f32)

    pending = []

    def send(*args):
        copy = remote(*args)
        copy.start()
        pending.append(copy)
        return copy

    mine_gu, mine_dn = block(me, rows_gu), block(me, rows_dn)
    loads[0].wait()
    gu_full[mine_gu, :hid] = weights[GATE][...].astype(bf16)
    loads[1].wait()
    gu_full[mine_gu, hid:] = weights[UP][...].astype(bf16)
    loads[2].wait()
    dn_full[mine_dn, :] = weights[DOWN][...].astype(bf16)

    pl.semaphore_wait(barrier, n_e + n_dp - 2)

    id_copies = [None] + [
        send(ids, all_ids.at[d], id_send.at[d], id_recv.at[d], {"expert": me_e ^ d}) for d in range(1, n_e)
    ]
    all_ids[0] = ids[...]

    fulls, shard_rows = (gu_full, dn_full), (rows_gu, rows_dn)

    def shard(part, origin):
        return fulls[part].at[block(origin, shard_rows[part])]

    def along(way, hop, part):
        side = 0 if way > 0 else 1
        origin = me - 2 * way * hop
        return remote(
            shard(part, origin), shard(part, origin),
            line_send.at[side, hop, part], line_recv.at[side, hop, part], {"dp": me + 2 * way},
        )

    def arriving(way, hop, part):
        side = 0 if way > 0 else 1
        origin = me - 2 * way * (hop + 1)
        return remote(
            shard(part, origin), shard(part, origin),
            line_send.at[side, hop, part], line_recv.at[side, hop, part], {"dp": me ^ 1},
        )

    def across(way, hop, part):
        side = 0 if way > 0 else 1
        origin = me - 2 * way * hop
        return remote(
            shard(part, origin), shard(part, origin),
            pair_send.at[side, hop, part], pair_recv.at[side, hop, part], {"dp": me ^ 1},
        )

    def across_arriving(way, hop, part):
        side = 0 if way > 0 else 1
        origin = (me ^ 1) - 2 * way * hop
        return remote(
            shard(part, origin), shard(part, origin),
            pair_send.at[side, hop, part], pair_recv.at[side, hop, part], {"dp": me ^ 1},
        )

    def has(way, hop):
        behind = chip >= hop if way > 0 else chip < chips - hop
        ahead = chip < chips - 1 if way > 0 else chip >= 1
        return behind, ahead

    for part in (0, 1):
        for way in (1, -1):
            @pl.when(has(way, 0)[1])
            def _(way=way, part=part):
                along(way, 0, part).start()
    for part in (0, 1):
        across(1, 0, part).start()

    def forward(hop, part):
        for way in (1, -1):
            behind, ahead = has(way, hop + 1)

            @pl.when(behind)
            def _(way=way):
                arriving(way, hop, part).wait_recv()

            @pl.when(jnp.logical_and(behind, ahead))
            def _(way=way):
                along(way, hop + 1, part).start()

            @pl.when(behind)
            def _(way=way):
                across(way, hop + 1, part).start()

    def crossed(hop, part):
        if hop == 0:
            across_arriving(1, 0, part).wait_recv()
            return
        for way in (1, -1):
            @pl.when(has(way, hop)[0])
            def _(way=way):
                across_arriving(way, hop, part).wait_recv()

    lane = lax.broadcasted_iota(jnp.int32, (slots, 128), 1)

    def chosen(d):
        column = jnp.transpose(jnp.broadcast_to(all_ids[d], (128, slots)))
        return jnp.concatenate(
            [jnp.where(column == lane + c * 128, 1.0, 0.0).astype(bf16) for c in range(pool_rows // 128)], axis=1
        )

    own_cols = block(me_e, width)
    loads[3].wait()
    for d in peers_e:
        id_copies[d].wait_recv()
        stage_x[d - 1] = dot(chosen(d), tokens[...]).astype(bf16)
        send(stage_x.at[d - 1], routed.at[:, own_cols], tok_send.at[d, 0], tok_recv.at[d, 0], {"expert": me_e ^ d})
    loads[4].wait()
    for d in peers_e:
        stage_c[d - 1] = dot(chosen(d), cot[...]).astype(bf16)
        send(stage_c.at[d - 1], cot_rows.at[:, own_cols], tok_send.at[d, 1], tok_recv.at[d, 1], {"expert": me_e ^ d})

    last_hop = chips - 1
    forward(0, 0)
    choice = chosen(0)
    routed[:, own_cols] = dot(choice, tokens[...]).astype(bf16)
    cot_rows[:, own_cols] = dot(choice, cot[...]).astype(bf16)
    forward(0, 1)

    route_column = jnp.transpose(jnp.broadcast_to(route[...], (128, slots)))

    def tokens_in(d, part):
        land = (routed, cot_rows)[part]
        theirs = block(me_e ^ d, width)
        stage = (stage_x, stage_c)[part]
        remote(
            stage.at[d - 1], land.at[:, theirs], tok_send.at[d, part], tok_recv.at[d, part], {"expert": me_e ^ d}
        ).wait_recv()

    def turn(d):
        e = me_e ^ d
        per = width // rows_gu
        flipped = jnp.transpose(routed[:, block(e, width)])
        for i in range(per):
            at = block(e * (per // 2) + i // 2, rows_gu)
            x_t[(i % 2) ^ core, at, :] = flipped[i * rows_gu : (i + 1) * rows_gu]

    def scale(d):
        for c in range(width // 128):
            at = pl.ds(pl.multiple_of((me_e ^ d) * width + c * 128, 128), 128)
            cot_rows[:, at] = (route_column * cot_rows[:, at].astype(f32)).astype(bf16)

    tall = min(256, slots)

    def multiply(origin, first):
        at = block(origin, 2 * rows_gu)
        for m in range(slots // tall):
            part = dot(routed[m * tall : (m + 1) * tall, at], gu_full[at, :])
            if first:
                pre[m * tall : (m + 1) * tall, :] = part
            else:
                pre[m * tall : (m + 1) * tall, :] += part

    def multiply_hop(hop):
        crossed(hop, 0)
        for way in (1, -1):
            @pl.when(has(way, hop)[0])
            def _(way=way):
                multiply(chip - way * hop, False)

    turn(0)
    scale(0)
    for d in peers_e:
        tokens_in(d, 0)
        turn(d)
    crossed(0, 0)
    multiply(chip, True)
    for hop in range(1, chips):
        if hop > 1:
            forward(hop - 1, 0)
        multiply_hop(hop)
        if 1 < hop < last_hop:
            forward(hop - 1, 1)

    step = 16

    def activate(i, carry):
        at = pl.ds(pl.multiple_of(i * step, step), step)
        gate_pre, up_pre = pre[at, :hid], pre[at, hid:]
        sig = jax.nn.sigmoid(gate_pre)
        act = gate_pre * sig
        hidden[at, :] = (act * up_pre).astype(bf16)
        pre[at, :hid] = up_pre * sig * (1.0 + gate_pre * (1.0 - sig))
        pre[at, hid:] = act
        return carry

    lax.fori_loop(0, slots // step, activate, 0, unroll=2)
    flipped = jnp.transpose(hidden[...])
    for p in range(n_dp):
        h_t[(p % 2) ^ core, (p // 2) * rows_dn : (p // 2 + 1) * rows_dn, :] = flipped[p * rows_dn : (p + 1) * rows_dn]

    offset = [(2 << t) - 2 - t for t in range(tiers)]
    flying, news, totals = {}, {}, {}

    def blocks_at(t):
        return n_dp >> (t + 1)

    def block_copy(m, t, k):
        size = blocks_at(t) // chunks_of(blocks_at(t)) * rows[m]
        at = pl.ds(k * size, size)
        src = sent[m] if t == 0 else outs[m][t - 1]
        return remote(
            src.at[at], ins[m][t].at[at], blk_send.at[m, t, k], blk_recv.at[m, t, k], {"dp": me ^ (1 << t)}
        )

    def launch_all(m, t, now=None):
        for k in range(chunks_of(blocks_at(t))):
            copy = block_copy(m, t, k)
            if now is None:
                copy.start()
            else:
                pl.when(now)(copy.start)
            if (m, t, k) not in flying:
                flying[m, t, k] = copy
                pending.append(copy)

    def gradient(m, away):
        total = half * rows[m]
        tile = min(256, total)
        parts = chunks_of(half)
        done = 0
        for i in range(total // tile):
            at = pl.ds(i * tile, tile)
            value = dot(x_t[1 if away else 0, at, :], both[:, m * hid : (m + 1) * hid]) * (1.0 / slots)
            if away:
                sent[m][at, :] = value.astype(bf16)
            else:
                own[m][at, :] = value
            while away and done < parts and (i + 1) * tile >= (done + 1) * (total // parts):
                flying[m, 0, done] = block_copy(m, 0, done)
                flying[m, 0, done].start()
                pending.append(flying[m, 0, done])
                done += 1

    down_copies = {}

    def gradient_down(d):
        at = block(me_e ^ d, width)
        sent[DOWN][:, at] = (dot(h_t[1], cot_rows[:, at]) * (1.0 / slots)).astype(bf16)
        down_copies[d] = send(
            sent[DOWN].at[:, at], ins[DOWN][0].at[:, at], dn_send.at[d], dn_recv.at[d], {"dp": me ^ 1}
        )
        own[DOWN][:, at] = dot(h_t[0], cot_rows[:, at]) * (1.0 / slots)

    def low(t):
        return lax.shift_right_logical(me, 1) & ((1 << t) - 1)

    def bit_of(t):
        return lax.shift_right_logical(me, t) & 1

    def fold(x):
        return x[:8] + x[8:]

    def lanes(x):
        total = x[:, :128]
        for c in range(1, x.shape[1] // 128):
            total = total + x[:, c * 128 : (c + 1) * 128]
        return jnp.sum(total, axis=0, keepdims=True)

    def measure(m, t):
        blocks, steps = blocks_at(t), rows[m] // step
        parts = chunks_of(blocks)
        bit, base = bit_of(t), low(t)
        acc = tuple(jnp.zeros((8, lump), f32) for _ in range(3))

        def body(places, i, acc):
            j, r = i // steps, i % steps
            at_mine = pl.ds(pl.multiple_of(((j << t) + base) * rows[m] + r * step, step), step)
            at_other = pl.ds(pl.multiple_of(i * step, step), step)
            ab, aa, bb = acc
            for at in places:
                a = own[m][at_mine, at]
                b = ins[m][t][at_other, at].astype(f32)
                ab, aa, bb = ab + fold(a * b), aa + fold(a * a), bb + fold(b * b)
            return ab, aa, bb

        if m == DOWN and t == 0:
            for d in (0, *peers_e):
                down_copies[d].wait_recv()
                first = (me_e ^ d) * width
                places = [pl.ds(pl.multiple_of(first + c, lump), lump) for c in range(0, width, lump)]
                acc = lax.fori_loop(0, blocks * steps, functools.partial(body, places), acc, unroll=2)
        else:
            per = blocks // parts * steps
            places = [pl.ds(c, lump) for c in range(0, cols[m], lump)]
            for k in range(parts):
                flying[m, t, k].wait_recv()
                acc = lax.fori_loop(
                    k * per, (k + 1) * per, functools.partial(body, places), acc, unroll=2 if per % 2 == 0 else 1
                )

        ab, aa, bb = (lanes(x) for x in acc)
        local = jnp.concatenate(
            [ab, jnp.where(bit == 0, aa, bb), jnp.where(bit == 0, bb, aa), jnp.zeros((5, 128), f32)], axis=0
        )
        stats[m, t] = local
        totals[m, t] = local
        news[m, t] = [
            send(
                stats.at[m, t], stats_in.at[m, offset[t] + d - 1],
                st_send.at[m, offset[t] + d - 1], st_recv.at[m, offset[t] + d - 1], {"dp": me ^ d},
            )
            for d in range(1, 2 << t)
        ]

    def settle(m, t):
        total = totals[m, t]
        for d in range(1, 2 << t):
            news[m, t][d - 1].wait_recv()
            total = total + stats_in[m, offset[t] + d - 1]
        whole = jnp.sum(total, axis=1, keepdims=True)
        inner, bit = whole[0:1], bit_of(t)
        c_left, c_right = coefs(inner, whole[1:2]), coefs(inner, whole[2:3])
        c_mine = jnp.where(bit == 0, c_left, c_right)
        c_other = jnp.where(bit == 0, c_right, c_left)
        return jnp.broadcast_to(c_mine, (1, lump)), jnp.broadcast_to(c_other, (1, lump))

    def combine(m, t, c_m, c_o, count, which, store):
        steps, base = rows[m] // step, low(t)

        def body(i, carry):
            jj, r = i // steps, i % steps
            j = which(jj)
            at_mine = pl.ds(pl.multiple_of(((j << t) + base) * rows[m] + r * step, step), step)
            at_other = pl.ds(pl.multiple_of(j * rows[m] + r * step, step), step)
            for c in range(0, cols[m], lump):
                value = own[m][at_mine, c : c + lump] * c_m
                value = value + ins[m][t][at_other, c : c + lump].astype(f32) * c_o
                store(i, at_mine, pl.ds(c, lump), value)
            return carry

        n = count * steps
        lax.fori_loop(0, n, body, 0, unroll=2 if n % 2 == 0 else 1)

    def merge(m, t):
        c_m, c_o = settle(m, t)
        up = bit_of(t + 1)
        count = blocks_at(t + 1)

        def store_away(i, at, to, value):
            outs[m][t][pl.ds(pl.multiple_of(i * step, step), step), to] = value.astype(bf16)

        def store_own(i, at, to, value):
            own[m][at, to] = value

        combine(m, t, c_m, c_o, count, lambda j: 2 * j + 1 - up, store_away)
        combine(m, t, c_m, c_o, count, lambda j: 2 * j + up, store_own)

    new, following = (new_gate, new_up, new_down), (next_gate, next_up, next_down)

    def finish(m):
        t = tiers - 1
        c_m, c_o = settle(m, t)
        loads[5 + m].wait()

        def store(i, at, to, value):
            row = pl.ds(pl.multiple_of(i * step, step), step)
            update(m, row, to, value)

        combine(m, t, c_m, c_o, 1, lambda j: j, store)

    def update(m, row, to, value):
        momentum = momentum_decay * moments[m][row, to] + value
        following[m][0, row, to] = momentum
        new[m][0, row, to] = weights[m][row, to] - learning_rate * momentum

    same_way = bit_of(1) == bit_of(2)
    other_way = jnp.logical_not(same_way)

    far = {}

    def scatter(m):
        c_m, c_o = settle(m, 0)
        for r in (3, 2, 1):
            def store_far(i, at, to, value, r=r):
                far_out[pl.ds(pl.multiple_of((r - 1) * rows[m] + i * step, step), step), to] = value.astype(bf16)

            combine(m, 0, c_m, c_o, 1, lambda j, r=r: chip ^ r, store_far)
            at = pl.ds((r - 1) * rows[m], rows[m])
            far[r] = remote(far_out.at[at], far_in.at[at], far_send.at[r - 1], far_recv.at[r - 1], {"dp": me ^ (2 * r)})
            pending.append(far[r])
            if r == 3:
                far[r].start()
            elif r == 2:
                pl.when(other_way)(far[r].start)

        def store_own(i, at, to, value):
            own[m][at, to] = value

        combine(m, 0, c_m, c_o, 1, lambda j: chip, store_own)

    def by_chip(swap, items):
        for b in (0, 1):
            bit = lax.shift_right_logical(chip, b) & 1
            items = {k: jnp.where(bit == 0, items[k], items[swap(k, 1 << b)]) for k in items}
        return items

    pairs4 = [(i, j) for i in range(4) for j in range(4)]

    def far_tiles(m, i, to):
        mine = pl.ds(pl.multiple_of(chip * rows[m] + i * step, step), step)
        tiles = [own[m][mine, to]]
        for r in (1, 2, 3):
            tiles.append(far_in[pl.ds(pl.multiple_of((r - 1) * rows[m] + i * step, step), step), to].astype(f32))
        return tiles

    def gram(m):
        for r in (1, 2, 3):
            far[r].wait_recv()
        wide = lump // 2
        upper = [(i, j) for i, j in pairs4 if i <= j]

        def body(i, acc):
            for c in range(0, cols[m], wide):
                v = far_tiles(m, i, pl.ds(c, wide))
                acc = tuple(x + fold(v[a] * v[b]) for x, (a, b) in zip(acc, upper))
            return acc

        acc = lax.fori_loop(0, rows[m] // step, body, tuple(jnp.zeros((8, wide), f32) for _ in upper))
        sums = {k: lanes(x) for k, x in zip(upper, acc)}
        sums = {(i, j): sums[min(i, j), max(i, j)] for i, j in pairs4}
        sums = by_chip(lambda k, s: (k[0] ^ s, k[1] ^ s), sums)
        local = jnp.concatenate([sums[k] for k in pairs4], axis=0)
        far_stats[...] = local
        totals[m, 1] = local
        news[m, 1] = [
            send(far_stats, far_stats_in.at[d - 1], table_send.at[d - 1], table_recv.at[d - 1], {"dp": me ^ d})
            for d in range(1, n_dp)
        ]

    def finish_far(m):
        total = totals[m, 1]
        for d in range(1, n_dp):
            news[m, 1][d - 1].wait_recv()
            total = total + far_stats_in[d - 1]
        whole = jnp.sum(total, axis=1, keepdims=True)
        g = {(i, j): whole[4 * i + j : 4 * i + j + 1] for i, j in pairs4}
        share = {}
        for a, b in ((0, 1), (2, 3)):
            share[a], share[b] = coefs(g[a, b], g[a, a]), coefs(g[a, b], g[b, b])

        def norm(a, b):
            value = share[a] * share[a] * g[a, a] + 2.0 * share[a] * share[b] * g[a, b] + share[b] * share[b] * g[b, b]
            return jnp.maximum(value, 0.0)

        inner = sum(share[a] * share[b] * g[a, b] for a in (0, 1) for b in (2, 3))
        c_left, c_right = coefs(inner, norm(0, 1)), coefs(inner, norm(2, 3))
        w = {a: share[a] * (c_left if a < 2 else c_right) for a in range(4)}
        w = by_chip(lambda k, s: k ^ s, w)
        w = [jnp.broadcast_to(w[r], (1, lump)) for r in range(4)]
        loads[5 + m].wait()

        def body(i, carry):
            row = pl.ds(pl.multiple_of(i * step, step), step)
            for c in range(0, cols[m], lump):
                to = pl.ds(c, lump)
                v = far_tiles(m, i, to)
                update(m, row, to, v[0] * w[0] + v[1] * w[1] + (v[2] * w[2] + v[3] * w[3]))
            return carry

        lax.fori_loop(0, rows[m] // step, body, 0, unroll=2)

    gradient_down(0)
    for d in peers_e:
        tokens_in(d, 1)
        scale(d)
        gradient_down(d)
    forward(last_hop - 1, 1)
    measure(DOWN, 0)
    for hop in range(chips):
        crossed(hop, 1)

    def backward(m):
        at = slice(m * tall, (m + 1) * tall)
        back = dot_t(cot_rows[at, :], dn_full[...])
        both[at, :hid] = (back * pre[at, :hid]).astype(bf16)
        both[at, hid:] = (back * pre[at, hid:]).astype(bf16)

    backward(0)
    straight = chips == 4
    if straight:
        scatter(DOWN)
    else:
        merge(DOWN, 0)
        launch_all(DOWN, 1)
    for m in range(1, slots // tall):
        backward(m)

    def slot_back(d):
        weight = gu_full[block(me_e ^ d, width), :]
        value = dot_t(both[...], weight).astype(bf16)
        if d == 0:
            returned[0:slots, :] = value
            return None
        slot_grad[d - 1] = value
        return send(
            slot_grad.at[d - 1], returned.at[pl.ds(d * slots, slots)], ret_send.at[d], ret_recv.at[d],
            {"expert": me_e ^ d},
        )

    def pool_sum():
        for copy in back_copies:
            copy.wait_recv()
        tile = 256

        @pl.loop(0, pool_rows // tile)
        def _(t):
            at = pl.multiple_of(t * tile, tile)
            row = lax.broadcasted_iota(jnp.int32, (tile, slots), 0) + at
            pick = jnp.concatenate(
                [jnp.where(row == all_ids[d], 1.0, 0.0).astype(bf16) for d in range(n_e)], axis=1
            )
            pool[pl.ds(at, tile), :] = dot(pick, returned[...])

    gradient(GATE, True)
    gradient(UP, True)
    gradient(GATE, False)
    measure(GATE, 0)
    gradient(UP, False)
    merge(GATE, 0)
    if straight:
        launch_all(GATE, 1)
        pl.when(same_way)(far[2].start)
    measure(UP, 0)
    back_copies = [slot_back(d) for d in peers_e]
    merge(UP, 0)
    slot_back(0)
    if straight:
        measure(GATE, 1)
        launch_all(UP, 1)
        merge(GATE, 1)
        launch_all(GATE, 2)
        measure(UP, 1)
        pl.when(other_way)(far[1].start)
        measure(GATE, 2)
        merge(UP, 1)
        launch_all(UP, 2)
        pl.when(same_way)(far[1].start)
        pool_sum()
        finish(GATE)
        gram(DOWN)
        measure(UP, 2)
        finish_far(DOWN)
        finish(UP)
    else:
        measure(DOWN, 1)
        launch_all(GATE, 1)
        merge(DOWN, 1)
        measure(GATE, 1)
        launch_all(DOWN, 2)
        launch_all(UP, 1)
        merge(GATE, 1)
        pool_sum()
        measure(UP, 1)
        launch_all(GATE, 2)
        merge(UP, 1)
        launch_all(UP, 2)
        for t in range(2, tiers):
            for m in (DOWN, GATE, UP):
                measure(m, t)
                if t == tiers - 1:
                    finish(m)
                else:
                    merge(m, t)
                    launch_all(m, t + 1)

    for part in (0, 1):
        across(1, 0, part).wait_send()
    for hop in range(chips):
        for part in (0, 1):
            for way in (1, -1):
                behind, ahead = has(way, hop)

                @pl.when(jnp.logical_and(behind, ahead))
                def _(way=way, hop=hop, part=part):
                    along(way, hop, part).wait_send()

                if hop:
                    @pl.when(behind)
                    def _(way=way, hop=hop, part=part):
                        across(way, hop, part).wait_send()
    for copy in pending:
        copy.wait_send()


def store_kernel(*refs):
    *pairs, sem = refs
    count = len(pairs) // 2
    copies = [pltpu.make_async_copy(pairs[i], pairs[count + i], sem.at[i]) for i in range(count)]
    for copy in copies:
        copy.start()
    for copy in copies:
        copy.wait()


def local(
    pool_tokens,
    pool_cotangent,
    token_ids,
    route_weights,
    gate_weight,
    up_weight,
    down_weight,
    momentum_gate,
    momentum_up,
    momentum_down,
):
    bf16, f32 = jnp.bfloat16, jnp.float32
    n_e, n_dp = lax.axis_size("expert"), lax.axis_size("dp")
    chips, half, tiers = n_dp // 2, n_dp // 2, n_dp.bit_length() - 1
    pool_rows, width = pool_tokens.shape
    slots = token_ids.shape[1]
    rows_gu, hid = gate_weight.shape[1:]
    rows_dn, full = down_weight.shape[1:]
    shapes = ((rows_gu, hid), (rows_gu, hid), (rows_dn, full))
    n_stats = sum((2 << t) - 1 for t in range(tiers))
    vmem, anywhere = pl.BlockSpec(memory_space=pltpu.VMEM), pl.BlockSpec(memory_space=pl.ANY)
    dma, buf = pltpu.SemaphoreType.DMA, pltpu.VMEM

    def per_matrix(blocks, kind):
        return [buf((blocks * r, c), kind) for r, c in shapes]

    def per_tier(first, kind):
        return [[buf(((n_dp >> (t + 1)) * r, c), kind) for t in range(first, tiers)] for r, c in shapes]

    like = [(x.shape, f32) for x in (gate_weight, up_weight, down_weight)]
    like = [*like, *like, ((pool_rows, width), f32)]
    results = pl.pallas_call(
        functools.partial(step_kernel, n_e, n_dp),
        out_shape=[buf(*x) for x in like],
        in_specs=[vmem] * 2 + [anywhere] * 8,
        out_specs=[vmem] * len(like),
        scratch_shapes=[
            buf((pool_rows, width), bf16),
            buf((pool_rows, width), bf16),
            per_matrix(1, f32),
            per_matrix(1, f32),
            buf((n_e, 1, slots), jnp.int32),
            buf((n_e - 1, slots, width), bf16),
            buf((n_e - 1, slots, width), bf16),
            buf((slots, full), bf16),
            buf((slots, full), bf16),
            buf((n_dp * rows_gu, 2 * hid), bf16),
            buf((n_dp * rows_dn, full), bf16),
            buf((2, half * rows_gu, slots), bf16),
            buf((2, half * rows_dn, slots), bf16),
            buf((slots, hid), bf16),
            buf((slots, 2 * hid), f32),
            buf((slots, 2 * hid), bf16),
            buf((n_e - 1, slots, width), bf16),
            buf((n_e * slots, width), bf16),
            per_matrix(half, f32),
            per_matrix(half, bf16),
            per_tier(1, bf16),
            per_tier(0, bf16),
            buf((3, tiers, 8, 128), f32),
            buf((3, n_stats, 8, 128), f32),
            buf((3 * rows_dn, full), bf16),
            buf((3 * rows_dn, full), bf16),
            buf((16, 128), f32),
            buf((7, 16, 128), f32),
            dma((8,)), dma((n_e,)), dma((n_e,)), dma((n_e, 2)), dma((n_e, 2)),
            dma((2, chips, 2)), dma((2, chips, 2)), dma((2, chips, 2)), dma((2, chips, 2)),
            dma((n_e,)), dma((n_e,)), dma((3, tiers, 2)), dma((3, tiers, 2)), dma((3, n_stats)), dma((3, n_stats)), dma((n_e,)), dma((n_e,)),
            dma((3,)), dma((3,)), dma((7,)), dma((7,)),
        ],
        compiler_params=pltpu.CompilerParams(
            collective_id=1, has_side_effects=True, vmem_limit_bytes=54 * 1024 * 1024
        ),
    )(
        token_ids, route_weights, pool_tokens, pool_cotangent, gate_weight, up_weight, down_weight,
        momentum_gate, momentum_up, momentum_down,
    )
    return pl.pallas_call(
        store_kernel,
        out_shape=[jax.ShapeDtypeStruct(*x) for x in like],
        in_specs=[vmem] * len(like),
        out_specs=[anywhere] * len(like),
        scratch_shapes=[dma((len(like),))],
        compiler_params=pltpu.CompilerParams(vmem_limit_bytes=1024 * 1024),
    )(*results)


def solution(mesh):
    in_specs = (
        P("dp", "expert"),
        P("dp", "expert"),
        P("expert", "dp"),
        P("expert", "dp"),
        P("expert", "dp", None),
        P("expert", "dp", None),
        P("expert", "dp", None),
        P("expert", "dp", None),
        P("expert", "dp", None),
        P("expert", "dp", None),
    )
    out_specs = (
        P("expert", "dp", None),
        P("expert", "dp", None),
        P("expert", "dp", None),
        P("expert", "dp", None),
        P("expert", "dp", None),
        P("expert", "dp", None),
        P("dp", "expert"),
    )
    return jax.shard_map(local, mesh=mesh, in_specs=in_specs, out_specs=out_specs, check_vma=False)
```

```python
import functools

import jax
import jax.numpy as jnp
from jax import lax
from jax.experimental import pallas as pl
from jax.experimental.pallas import tpu as pltpu
from jax.sharding import PartitionSpec as P


momentum_decay = 0.9
learning_rate = 0.05
epsilon = 1e-06
GATE, UP, DOWN = 0, 1, 2


def coefs(inner, norm):
    return 1.0 - inner / (2.0 * (norm + epsilon))


def chunks_of(blocks):
    return min(2, blocks)


def step_kernel(
    n_e, n_dp,
    ids, route, tok_h, cot_h, gate_h, up_h, down_h, mom_gate_h, mom_up_h, mom_down_h,
    new_gate, new_up, new_down, next_gate, next_up, next_down, pool,
    tokens, cot, weights, moments, all_ids, stage_x, stage_c, routed, cot_rows,
    gu_full, dn_full, x_t, h_t, hidden, pre, both, slot_grad, returned,
    own, sent, outs, ins, stats, stats_in, far_out, far_in, far_stats, far_stats_in,
    in_sem, id_send, id_recv, tok_send, tok_recv, line_send, line_recv, pair_send, pair_recv,
    ret_send, ret_recv, blk_send, blk_recv, st_send, st_recv, dn_send, dn_recv,
    far_send, far_recv, table_send, table_recv,
):
    f32, bf16 = jnp.float32, jnp.bfloat16
    MESH = pl.DeviceIdType.MESH
    me, me_e = lax.axis_index("dp"), lax.axis_index("expert")
    chips = n_dp // 2
    chip, core = me // 2, me % 2
    tiers = n_dp.bit_length() - 1
    half = n_dp // 2
    slots = ids.shape[1]
    pool_rows, width = tokens.shape
    hid = pre.shape[1] // 2
    rows_gu, rows_dn = gate_h.shape[1], down_h.shape[1]
    rows = (rows_gu, rows_gu, rows_dn)
    cols = (hid, hid, down_h.shape[2])
    lump = min(512, hid)
    peers_e = sorted(range(1, n_e), key=lambda d: -bin(d).count("1"))

    barrier = pltpu.get_barrier_semaphore()
    for d in range(1, n_e):
        pl.semaphore_signal(barrier, inc=1, device_id={"expert": me_e ^ d}, device_id_type=MESH)
    for d in range(1, n_dp):
        pl.semaphore_signal(barrier, inc=1, device_id={"dp": me ^ d}, device_id_type=MESH)

    loads = [
        pltpu.make_async_copy(src, dst, in_sem.at[i])
        for i, (src, dst) in enumerate(
            (
                (gate_h.at[0], weights[GATE]), (up_h.at[0], weights[UP]), (down_h.at[0], weights[DOWN]),
                (tok_h, tokens), (cot_h, cot),
                (mom_gate_h.at[0], moments[GATE]), (mom_up_h.at[0], moments[UP]), (mom_down_h.at[0], moments[DOWN]),
            )
        )
    ]
    for copy in loads:
        copy.start()

    def remote(src, dst, ssem, rsem, device):
        return pltpu.make_async_remote_copy(
            src_ref=src, dst_ref=dst, send_sem=ssem, recv_sem=rsem, device_id=device, device_id_type=MESH
        )

    def block(index, size):
        return pl.ds(pl.multiple_of(index * size, size), size)

    def dot(a, b):
        return jnp.dot(a, b, preferred_element_type=f32)

    def dot_t(a, b):
        return lax.dot_general(a, b, (((1,), (1,)), ((), ())), preferred_element_type=f32)

    pending = []

    def send(*args):
        copy = remote(*args)
        copy.start()
        pending.append(copy)
        return copy

    mine_gu, mine_dn = block(me, rows_gu), block(me, rows_dn)
    loads[0].wait()
    gu_full[mine_gu, :hid] = weights[GATE][...].astype(bf16)
    loads[1].wait()
    gu_full[mine_gu, hid:] = weights[UP][...].astype(bf16)
    loads[2].wait()
    dn_full[mine_dn, :] = weights[DOWN][...].astype(bf16)

    pl.semaphore_wait(barrier, n_e + n_dp - 2)

    id_copies = [None] + [
        send(ids, all_ids.at[d], id_send.at[d], id_recv.at[d], {"expert": me_e ^ d}) for d in range(1, n_e)
    ]
    all_ids[0] = ids[...]

    fulls, shard_rows = (gu_full, dn_full), (rows_gu, rows_dn)

    def shard(part, origin):
        return fulls[part].at[block(origin, shard_rows[part])]

    def along(way, hop, part):
        side = 0 if way > 0 else 1
        origin = me - 2 * way * hop
        return remote(
            shard(part, origin), shard(part, origin),
            line_send.at[side, hop, part], line_recv.at[side, hop, part], {"dp": me + 2 * way},
        )

    def arriving(way, hop, part):
        side = 0 if way > 0 else 1
        origin = me - 2 * way * (hop + 1)
        return remote(
            shard(part, origin), shard(part, origin),
            line_send.at[side, hop, part], line_recv.at[side, hop, part], {"dp": me ^ 1},
        )

    def across(way, hop, part):
        side = 0 if way > 0 else 1
        origin = me - 2 * way * hop
        return remote(
            shard(part, origin), shard(part, origin),
            pair_send.at[side, hop, part], pair_recv.at[side, hop, part], {"dp": me ^ 1},
        )

    def across_arriving(way, hop, part):
        side = 0 if way > 0 else 1
        origin = (me ^ 1) - 2 * way * hop
        return remote(
            shard(part, origin), shard(part, origin),
            pair_send.at[side, hop, part], pair_recv.at[side, hop, part], {"dp": me ^ 1},
        )

    def has(way, hop):
        behind = chip >= hop if way > 0 else chip < chips - hop
        ahead = chip < chips - 1 if way > 0 else chip >= 1
        return behind, ahead

    for part in (0, 1):
        for way in (1, -1):
            @pl.when(has(way, 0)[1])
            def _(way=way, part=part):
                along(way, 0, part).start()
    for part in (0, 1):
        across(1, 0, part).start()

    def forward(hop, part):
        for way in (1, -1):
            behind, ahead = has(way, hop + 1)

            @pl.when(behind)
            def _(way=way):
                arriving(way, hop, part).wait_recv()

            @pl.when(jnp.logical_and(behind, ahead))
            def _(way=way):
                along(way, hop + 1, part).start()

            @pl.when(behind)
            def _(way=way):
                across(way, hop + 1, part).start()

    def crossed(hop, part):
        if hop == 0:
            across_arriving(1, 0, part).wait_recv()
            return
        for way in (1, -1):
            @pl.when(has(way, hop)[0])
            def _(way=way):
                across_arriving(way, hop, part).wait_recv()

    lane = lax.broadcasted_iota(jnp.int32, (slots, 128), 1)

    def chosen(d, first=0, count=slots):
        column = jnp.transpose(jnp.broadcast_to(all_ids[d][:, first : first + count], (128, count)))
        return jnp.concatenate(
            [jnp.where(column == lane[:count] + c * 128, 1.0, 0.0).astype(bf16) for c in range(pool_rows // 128)],
            axis=1,
        )

    own_cols = block(me_e, width)
    pieces = ((0, slots // 4), (slots // 4, slots - slots // 4))

    def tokens_out(d, i):
        at = pl.ds(*pieces[i])
        stage_x[d - 1, at, :] = dot(chosen(d, *pieces[i]), tokens[...]).astype(bf16)
        send(
            stage_x.at[d - 1, at], routed.at[at, own_cols], tok_send.at[d, i], tok_recv.at[d, i], {"expert": me_e ^ d}
        )

    loads[3].wait()
    near = [d for d in range(1, n_e) if d & (d - 1) == 0]
    for i in (0, 1):
        for d in near:
            if i == 0:
                id_copies[d].wait_recv()
            tokens_out(d, i)
    for d in range(1, n_e):
        if d not in near:
            id_copies[d].wait_recv()
            tokens_out(d, 0)
            tokens_out(d, 1)
    loads[4].wait()
    for d in range(1, n_e):
        stage_c[d - 1] = dot(chosen(d), cot[...]).astype(bf16)
        send(stage_c.at[d - 1], cot_rows.at[:, own_cols], tok_send.at[d, 2], tok_recv.at[d, 2], {"expert": me_e ^ d})

    last_hop = chips - 1
    forward(0, 0)
    choice = chosen(0)
    routed[:, own_cols] = dot(choice, tokens[...]).astype(bf16)
    cot_rows[:, own_cols] = dot(choice, cot[...]).astype(bf16)
    forward(0, 1)

    route_column = jnp.transpose(jnp.broadcast_to(route[...], (128, slots)))

    def tokens_in(d, part):
        theirs, peer = block(me_e ^ d, width), {"expert": me_e ^ d}
        if part:
            remote(
                stage_c.at[d - 1], cot_rows.at[:, theirs], tok_send.at[d, 2], tok_recv.at[d, 2], peer
            ).wait_recv()
            return
        for i in (0, 1):
            at = pl.ds(*pieces[i])
            remote(
                stage_x.at[d - 1, at], routed.at[at, theirs], tok_send.at[d, i], tok_recv.at[d, i], peer
            ).wait_recv()

    def turn(d):
        e = me_e ^ d
        per = width // rows_gu
        flipped = jnp.transpose(routed[:, block(e, width)])
        for i in range(per):
            at = block(e * (per // 2) + i // 2, rows_gu)
            x_t[(i % 2) ^ core, at, :] = flipped[i * rows_gu : (i + 1) * rows_gu]

    def scale(d):
        for c in range(width // 128):
            at = pl.ds(pl.multiple_of((me_e ^ d) * width + c * 128, 128), 128)
            cot_rows[:, at] = (route_column * cot_rows[:, at].astype(f32)).astype(bf16)

    tall = min(256, slots)

    def multiply(origin, first):
        at = block(origin, 2 * rows_gu)
        for m in range(slots // tall):
            part = dot(routed[m * tall : (m + 1) * tall, at], gu_full[at, :])
            if first:
                pre[m * tall : (m + 1) * tall, :] = part
            else:
                pre[m * tall : (m + 1) * tall, :] += part

    def multiply_hop(hop):
        crossed(hop, 0)
        for way in (1, -1):
            @pl.when(has(way, hop)[0])
            def _(way=way):
                multiply(chip - way * hop, False)

    turn(0)
    scale(0)
    for d in range(1, n_e):
        tokens_in(d, 0)
        turn(d)
    crossed(0, 0)
    multiply(chip, True)
    for hop in range(1, chips):
        if hop == last_hop:
            tokens_in(1, 1)
            scale(1)
        if hop > 1:
            forward(hop - 1, 0)
        multiply_hop(hop)
        if 1 < hop < last_hop:
            forward(hop - 1, 1)

    step = 16

    def activate(i, carry):
        at = pl.ds(pl.multiple_of(i * step, step), step)
        gate_pre, up_pre = pre[at, :hid], pre[at, hid:]
        sig = jax.nn.sigmoid(gate_pre)
        act = gate_pre * sig
        hidden[at, :] = (act * up_pre).astype(bf16)
        pre[at, :hid] = up_pre * sig * (1.0 + gate_pre * (1.0 - sig))
        pre[at, hid:] = act
        return carry

    lax.fori_loop(0, slots // step, activate, 0, unroll=2)
    flipped = jnp.transpose(hidden[...])
    for p in range(n_dp):
        h_t[(p % 2) ^ core, (p // 2) * rows_dn : (p // 2 + 1) * rows_dn, :] = flipped[p * rows_dn : (p + 1) * rows_dn]

    offset = [(2 << t) - 2 - t for t in range(tiers)]
    flying, news, totals = {}, {}, {}

    def blocks_at(t):
        return n_dp >> (t + 1)

    def block_copy(m, t, k):
        size = blocks_at(t) // chunks_of(blocks_at(t)) * rows[m]
        at = pl.ds(k * size, size)
        src = sent[m] if t == 0 else outs[m][t - 1]
        return remote(
            src.at[at], ins[m][t].at[at], blk_send.at[m, t, k], blk_recv.at[m, t, k], {"dp": me ^ (1 << t)}
        )

    def launch_all(m, t, now=None):
        for k in range(chunks_of(blocks_at(t))):
            copy = block_copy(m, t, k)
            if now is None:
                copy.start()
            else:
                pl.when(now)(copy.start)
            if (m, t, k) not in flying:
                flying[m, t, k] = copy
                pending.append(copy)

    def gradient(m, away):
        total = half * rows[m]
        tile = min(256, total)
        parts = chunks_of(half)
        done = 0
        for i in range(total // tile):
            at = pl.ds(i * tile, tile)
            value = dot(x_t[1 if away else 0, at, :], both[:, m * hid : (m + 1) * hid]) * (1.0 / slots)
            if away:
                sent[m][at, :] = value.astype(bf16)
            else:
                own[m][at, :] = value
            while away and done < parts and (i + 1) * tile >= (done + 1) * (total // parts):
                flying[m, 0, done] = block_copy(m, 0, done)
                flying[m, 0, done].start()
                pending.append(flying[m, 0, done])
                done += 1

    down_copies = {}

    def down_away(d):
        at = block(me_e ^ d, width)
        sent[DOWN][:, at] = (dot(h_t[1], cot_rows[:, at]) * (1.0 / slots)).astype(bf16)
        down_copies[d] = send(
            sent[DOWN].at[:, at], ins[DOWN][0].at[:, at], dn_send.at[d], dn_recv.at[d], {"dp": me ^ 1}
        )

    def down_own(d):
        at = block(me_e ^ d, width)
        own[DOWN][:, at] = dot(h_t[0], cot_rows[:, at]) * (1.0 / slots)

    def low(t):
        return lax.shift_right_logical(me, 1) & ((1 << t) - 1)

    def bit_of(t):
        return lax.shift_right_logical(me, t) & 1

    def fold(x):
        return x[:8] + x[8:]

    def lanes(x):
        total = x[:, :128]
        for c in range(1, x.shape[1] // 128):
            total = total + x[:, c * 128 : (c + 1) * 128]
        return jnp.sum(total, axis=0, keepdims=True)

    def measure(m, t):
        blocks, steps = blocks_at(t), rows[m] // step
        parts = chunks_of(blocks)
        bit, base = bit_of(t), low(t)
        acc = tuple(jnp.zeros((8, lump), f32) for _ in range(3))

        def body(places, i, acc):
            j, r = i // steps, i % steps
            at_mine = pl.ds(pl.multiple_of(((j << t) + base) * rows[m] + r * step, step), step)
            at_other = pl.ds(pl.multiple_of(i * step, step), step)
            ab, aa, bb = acc
            for at in places:
                a = own[m][at_mine, at]
                b = ins[m][t][at_other, at].astype(f32)
                ab, aa, bb = ab + fold(a * b), aa + fold(a * a), bb + fold(b * b)
            return ab, aa, bb

        if m == DOWN and t == 0:
            for d in range(n_e):
                down_copies[d].wait_recv()
                first = (me_e ^ d) * width
                places = [pl.ds(pl.multiple_of(first + c, lump), lump) for c in range(0, width, lump)]
                acc = lax.fori_loop(0, blocks * steps, functools.partial(body, places), acc, unroll=2)
        else:
            per = blocks // parts * steps
            places = [pl.ds(c, lump) for c in range(0, cols[m], lump)]
            for k in range(parts):
                flying[m, t, k].wait_recv()
                acc = lax.fori_loop(
                    k * per, (k + 1) * per, functools.partial(body, places), acc, unroll=2 if per % 2 == 0 else 1
                )

        ab, aa, bb = (lanes(x) for x in acc)
        local = jnp.concatenate(
            [ab, jnp.where(bit == 0, aa, bb), jnp.where(bit == 0, bb, aa), jnp.zeros((5, 128), f32)], axis=0
        )
        stats[m, t] = local
        totals[m, t] = local
        news[m, t] = [
            send(
                stats.at[m, t], stats_in.at[m, offset[t] + d - 1],
                st_send.at[m, offset[t] + d - 1], st_recv.at[m, offset[t] + d - 1], {"dp": me ^ d},
            )
            for d in range(1, 2 << t)
        ]

    def settle(m, t):
        total = totals[m, t]
        for d in range(1, 2 << t):
            news[m, t][d - 1].wait_recv()
            total = total + stats_in[m, offset[t] + d - 1]
        whole = jnp.sum(total, axis=1, keepdims=True)
        inner, bit = whole[0:1], bit_of(t)
        c_left, c_right = coefs(inner, whole[1:2]), coefs(inner, whole[2:3])
        c_mine = jnp.where(bit == 0, c_left, c_right)
        c_other = jnp.where(bit == 0, c_right, c_left)
        return jnp.broadcast_to(c_mine, (1, lump)), jnp.broadcast_to(c_other, (1, lump))

    def combine(m, t, c_m, c_o, count, which, store):
        steps, base = rows[m] // step, low(t)

        def body(i, carry):
            jj, r = i // steps, i % steps
            j = which(jj)
            at_mine = pl.ds(pl.multiple_of(((j << t) + base) * rows[m] + r * step, step), step)
            at_other = pl.ds(pl.multiple_of(j * rows[m] + r * step, step), step)
            for c in range(0, cols[m], lump):
                value = own[m][at_mine, c : c + lump] * c_m
                value = value + ins[m][t][at_other, c : c + lump].astype(f32) * c_o
                store(i, at_mine, pl.ds(c, lump), value)
            return carry

        n = count * steps
        lax.fori_loop(0, n, body, 0, unroll=2 if n % 2 == 0 else 1)

    def merge(m, t, then=None):
        c_m, c_o = settle(m, t)
        up = bit_of(t + 1)
        count = blocks_at(t + 1)

        def store_away(i, at, to, value):
            outs[m][t][pl.ds(pl.multiple_of(i * step, step), step), to] = value.astype(bf16)

        def store_own(i, at, to, value):
            own[m][at, to] = value

        combine(m, t, c_m, c_o, count, lambda j: 2 * j + 1 - up, store_away)
        if then is not None:
            then()
        combine(m, t, c_m, c_o, count, lambda j: 2 * j + up, store_own)

    new, following = (new_gate, new_up, new_down), (next_gate, next_up, next_down)

    def finish(m):
        t = tiers - 1
        c_m, c_o = settle(m, t)
        loads[5 + m].wait()

        def store(i, at, to, value):
            row = pl.ds(pl.multiple_of(i * step, step), step)
            update(m, row, to, value)

        combine(m, t, c_m, c_o, 1, lambda j: j, store)

    def update(m, row, to, value):
        momentum = momentum_decay * moments[m][row, to] + value
        following[m][0, row, to] = momentum
        new[m][0, row, to] = weights[m][row, to] - learning_rate * momentum

    same_way = bit_of(1) == bit_of(2)
    other_way = jnp.logical_not(same_way)

    far = {}

    def scatter(m):
        c_m, c_o = settle(m, 0)
        for r in (2, 3, 1):
            def store_far(i, at, to, value, r=r):
                far_out[pl.ds(pl.multiple_of((r - 1) * rows[m] + i * step, step), step), to] = value.astype(bf16)

            combine(m, 0, c_m, c_o, 1, lambda j, r=r: chip ^ r, store_far)
            at = pl.ds((r - 1) * rows[m], rows[m])
            far[r] = remote(far_out.at[at], far_in.at[at], far_send.at[r - 1], far_recv.at[r - 1], {"dp": me ^ (2 * r)})
            pending.append(far[r])
            if r == 3:
                pl.when(other_way)(far[2].start)
                far[3].start()

        def store_own(i, at, to, value):
            own[m][at, to] = value

        combine(m, 0, c_m, c_o, 1, lambda j: chip, store_own)

    def by_chip(swap, items):
        for b in (0, 1):
            bit = lax.shift_right_logical(chip, b) & 1
            items = {k: jnp.where(bit == 0, items[k], items[swap(k, 1 << b)]) for k in items}
        return items

    pairs4 = [(i, j) for i in range(4) for j in range(4)]

    def far_tiles(m, i, to):
        mine = pl.ds(pl.multiple_of(chip * rows[m] + i * step, step), step)
        tiles = [own[m][mine, to]]
        for r in (1, 2, 3):
            tiles.append(far_in[pl.ds(pl.multiple_of((r - 1) * rows[m] + i * step, step), step), to].astype(f32))
        return tiles

    def gram(m):
        for r in (1, 2, 3):
            far[r].wait_recv()
        wide = lump // 2
        upper = [(i, j) for i, j in pairs4 if i <= j]

        def body(i, acc):
            for c in range(0, cols[m], wide):
                v = far_tiles(m, i, pl.ds(c, wide))
                acc = tuple(x + fold(v[a] * v[b]) for x, (a, b) in zip(acc, upper))
            return acc

        acc = lax.fori_loop(0, rows[m] // step, body, tuple(jnp.zeros((8, wide), f32) for _ in upper))
        sums = {k: lanes(x) for k, x in zip(upper, acc)}
        sums = {(i, j): sums[min(i, j), max(i, j)] for i, j in pairs4}
        sums = by_chip(lambda k, s: (k[0] ^ s, k[1] ^ s), sums)
        local = jnp.concatenate([sums[k] for k in pairs4], axis=0)
        far_stats[...] = local
        totals[m, 1] = local
        news[m, 1] = [
            send(far_stats, far_stats_in.at[d - 1], table_send.at[d - 1], table_recv.at[d - 1], {"dp": me ^ d})
            for d in range(1, n_dp)
        ]

    def finish_far(m):
        total = totals[m, 1]
        for d in range(1, n_dp):
            news[m, 1][d - 1].wait_recv()
            total = total + far_stats_in[d - 1]
        whole = jnp.sum(total, axis=1, keepdims=True)
        g = {(i, j): whole[4 * i + j : 4 * i + j + 1] for i, j in pairs4}
        share = {}
        for a, b in ((0, 1), (2, 3)):
            share[a], share[b] = coefs(g[a, b], g[a, a]), coefs(g[a, b], g[b, b])

        def norm(a, b):
            value = share[a] * share[a] * g[a, a] + 2.0 * share[a] * share[b] * g[a, b] + share[b] * share[b] * g[b, b]
            return jnp.maximum(value, 0.0)

        inner = sum(share[a] * share[b] * g[a, b] for a in (0, 1) for b in (2, 3))
        c_left, c_right = coefs(inner, norm(0, 1)), coefs(inner, norm(2, 3))
        w = {a: share[a] * (c_left if a < 2 else c_right) for a in range(4)}
        w = by_chip(lambda k, s: k ^ s, w)
        w = [jnp.broadcast_to(w[r], (1, lump)) for r in range(4)]
        loads[5 + m].wait()

        def body(i, carry):
            row = pl.ds(pl.multiple_of(i * step, step), step)
            for c in range(0, cols[m], lump):
                to = pl.ds(c, lump)
                v = far_tiles(m, i, to)
                update(m, row, to, v[0] * w[0] + v[1] * w[1] + (v[2] * w[2] + v[3] * w[3]))
            return carry

        lax.fori_loop(0, rows[m] // step, body, 0, unroll=2)

    down_away(0)
    for d in range(1, n_e):
        if d > 1:
            tokens_in(d, 1)
            scale(d)
        down_away(d)
    for d in range(n_e):
        down_own(d)
    forward(last_hop - 1, 1)
    measure(DOWN, 0)
    straight = chips == 4
    if straight:
        scatter(DOWN)
    else:
        merge(DOWN, 0)
        launch_all(DOWN, 1)

    for hop in range(chips):
        crossed(hop, 1)
    for m in range(slots // tall):
        at = slice(m * tall, (m + 1) * tall)
        back = dot_t(cot_rows[at, :], dn_full[...])
        both[at, :hid] = (back * pre[at, :hid]).astype(bf16)
        both[at, hid:] = (back * pre[at, hid:]).astype(bf16)

    def slot_back(d):
        weight = gu_full[block(me_e ^ d, width), :]
        value = dot_t(both[...], weight).astype(bf16)
        if d == 0:
            returned[0:slots, :] = value
            return None
        slot_grad[d - 1] = value
        return send(
            slot_grad.at[d - 1], returned.at[pl.ds(d * slots, slots)], ret_send.at[d], ret_recv.at[d],
            {"expert": me_e ^ d},
        )

    def pool_sum():
        for copy in back_copies:
            copy.wait_recv()
        tile = 256

        @pl.loop(0, pool_rows // tile)
        def _(t):
            at = pl.multiple_of(t * tile, tile)
            row = lax.broadcasted_iota(jnp.int32, (tile, slots), 0) + at
            pick = jnp.concatenate(
                [jnp.where(row == all_ids[d], 1.0, 0.0).astype(bf16) for d in range(n_e)], axis=1
            )
            pool[pl.ds(at, tile), :] = dot(pick, returned[...])

    gradient(GATE, True)
    gradient(GATE, False)
    gradient(UP, True)
    gradient(UP, False)
    measure(GATE, 0)

    def first_gate():
        if straight:
            launch_all(GATE, 1)
            pl.when(same_way)(far[2].start)

    merge(GATE, 0, first_gate)
    measure(UP, 0)
    back_copies = [slot_back(d) for d in peers_e]
    merge(UP, 0)
    slot_back(0)
    if straight:
        measure(GATE, 1)
        launch_all(UP, 1)
        merge(GATE, 1, lambda: launch_all(GATE, 2))
        measure(UP, 1)
        pl.when(other_way)(far[1].start)
        merge(UP, 1, lambda: launch_all(UP, 2))
        pl.when(same_way)(far[1].start)
        pool_sum()
        measure(GATE, 2)
        gram(DOWN)
        measure(UP, 2)
        finish(GATE)
        finish_far(DOWN)
        finish(UP)
    else:
        measure(DOWN, 1)
        launch_all(GATE, 1)
        merge(DOWN, 1)
        measure(GATE, 1)
        launch_all(DOWN, 2)
        launch_all(UP, 1)
        merge(GATE, 1)
        pool_sum()
        measure(UP, 1)
        launch_all(GATE, 2)
        merge(UP, 1)
        launch_all(UP, 2)
        for t in range(2, tiers):
            for m in (DOWN, GATE, UP):
                measure(m, t)
                if t == tiers - 1:
                    finish(m)
                else:
                    merge(m, t)
                    launch_all(m, t + 1)

    for part in (0, 1):
        across(1, 0, part).wait_send()
    for hop in range(chips):
        for part in (0, 1):
            for way in (1, -1):
                behind, ahead = has(way, hop)

                @pl.when(jnp.logical_and(behind, ahead))
                def _(way=way, hop=hop, part=part):
                    along(way, hop, part).wait_send()

                if hop:
                    @pl.when(behind)
                    def _(way=way, hop=hop, part=part):
                        across(way, hop, part).wait_send()
    for copy in pending:
        copy.wait_send()


def store_kernel(*refs):
    *pairs, sem = refs
    count = len(pairs) // 2
    copies = [pltpu.make_async_copy(pairs[i], pairs[count + i], sem.at[i]) for i in range(count)]
    for copy in copies:
        copy.start()
    for copy in copies:
        copy.wait()


def local(
    pool_tokens,
    pool_cotangent,
    token_ids,
    route_weights,
    gate_weight,
    up_weight,
    down_weight,
    momentum_gate,
    momentum_up,
    momentum_down,
):
    bf16, f32 = jnp.bfloat16, jnp.float32
    n_e, n_dp = lax.axis_size("expert"), lax.axis_size("dp")
    chips, half, tiers = n_dp // 2, n_dp // 2, n_dp.bit_length() - 1
    pool_rows, width = pool_tokens.shape
    slots = token_ids.shape[1]
    rows_gu, hid = gate_weight.shape[1:]
    rows_dn, full = down_weight.shape[1:]
    shapes = ((rows_gu, hid), (rows_gu, hid), (rows_dn, full))
    n_stats = sum((2 << t) - 1 for t in range(tiers))
    vmem, anywhere = pl.BlockSpec(memory_space=pltpu.VMEM), pl.BlockSpec(memory_space=pl.ANY)
    dma, buf = pltpu.SemaphoreType.DMA, pltpu.VMEM

    def per_matrix(blocks, kind):
        return [buf((blocks * r, c), kind) for r, c in shapes]

    def per_tier(first, kind):
        return [[buf(((n_dp >> (t + 1)) * r, c), kind) for t in range(first, tiers)] for r, c in shapes]

    like = [(x.shape, f32) for x in (gate_weight, up_weight, down_weight)]
    like = [*like, *like, ((pool_rows, width), f32)]
    results = pl.pallas_call(
        functools.partial(step_kernel, n_e, n_dp),
        out_shape=[buf(*x) for x in like],
        in_specs=[vmem] * 2 + [anywhere] * 8,
        out_specs=[vmem] * len(like),
        scratch_shapes=[
            buf((pool_rows, width), bf16),
            buf((pool_rows, width), bf16),
            per_matrix(1, f32),
            per_matrix(1, f32),
            buf((n_e, 1, slots), jnp.int32),
            buf((n_e - 1, slots, width), bf16),
            buf((n_e - 1, slots, width), bf16),
            buf((slots, full), bf16),
            buf((slots, full), bf16),
            buf((n_dp * rows_gu, 2 * hid), bf16),
            buf((n_dp * rows_dn, full), bf16),
            buf((2, half * rows_gu, slots), bf16),
            buf((2, half * rows_dn, slots), bf16),
            buf((slots, hid), bf16),
            buf((slots, 2 * hid), f32),
            buf((slots, 2 * hid), bf16),
            buf((n_e - 1, slots, width), bf16),
            buf((n_e * slots, width), bf16),
            per_matrix(half, f32),
            per_matrix(half, bf16),
            per_tier(1, bf16),
            per_tier(0, bf16),
            buf((3, tiers, 8, 128), f32),
            buf((3, n_stats, 8, 128), f32),
            buf((3 * rows_dn, full), bf16),
            buf((3 * rows_dn, full), bf16),
            buf((16, 128), f32),
            buf((7, 16, 128), f32),
            dma((8,)), dma((n_e,)), dma((n_e,)), dma((n_e, 3)), dma((n_e, 3)),
            dma((2, chips, 2)), dma((2, chips, 2)), dma((2, chips, 2)), dma((2, chips, 2)),
            dma((n_e,)), dma((n_e,)), dma((3, tiers, 2)), dma((3, tiers, 2)), dma((3, n_stats)), dma((3, n_stats)), dma((n_e,)), dma((n_e,)),
            dma((3,)), dma((3,)), dma((7,)), dma((7,)),
        ],
        compiler_params=pltpu.CompilerParams(
            collective_id=1, has_side_effects=True, vmem_limit_bytes=54 * 1024 * 1024
        ),
    )(
        token_ids, route_weights, pool_tokens, pool_cotangent, gate_weight, up_weight, down_weight,
        momentum_gate, momentum_up, momentum_down,
    )
    return pl.pallas_call(
        store_kernel,
        out_shape=[jax.ShapeDtypeStruct(*x) for x in like],
        in_specs=[vmem] * len(like),
        out_specs=[anywhere] * len(like),
        scratch_shapes=[dma((len(like),))],
        compiler_params=pltpu.CompilerParams(vmem_limit_bytes=1024 * 1024),
    )(*results)


def solution(mesh):
    in_specs = (
        P("dp", "expert"),
        P("dp", "expert"),
        P("expert", "dp"),
        P("expert", "dp"),
        P("expert", "dp", None),
        P("expert", "dp", None),
        P("expert", "dp", None),
        P("expert", "dp", None),
        P("expert", "dp", None),
        P("expert", "dp", None),
    )
    out_specs = (
        P("expert", "dp", None),
        P("expert", "dp", None),
        P("expert", "dp", None),
        P("expert", "dp", None),
        P("expert", "dp", None),
        P("expert", "dp", None),
        P("dp", "expert"),
    )
    return jax.shard_map(local, mesh=mesh, in_specs=in_specs, out_specs=out_specs, check_vma=False)
```

```python
import functools

import jax
import jax.numpy as jnp
from jax import lax
from jax.experimental import pallas as pl
from jax.experimental.pallas import tpu as pltpu
from jax.sharding import PartitionSpec as P


momentum_decay = 0.9
learning_rate = 0.05
epsilon = 1e-06
GATE, UP, DOWN = 0, 1, 2


def coefs(inner, norm):
    return 1.0 - inner / (2.0 * (norm + epsilon))


def chunks_of(blocks):
    return min(2, blocks)


def step_kernel(
    n_e, n_dp,
    ids, route, tok_h, cot_h, gate_h, up_h, down_h, mom_gate_h, mom_up_h, mom_down_h,
    new_gate, new_up, new_down, next_gate, next_up, next_down, pool,
    tokens, cot, weights, moments, all_ids, stage_x, stage_c, routed, cot_rows,
    gu_full, dn_full, x_t, h_t, hidden, pre, both, slot_grad, returned,
    own, sent, outs, ins, stats, stats_in, far_out, far_in, far_stats, far_stats_in,
    in_sem, id_send, id_recv, tok_send, tok_recv, line_send, line_recv, pair_send, pair_recv,
    ret_send, ret_recv, blk_send, blk_recv, st_send, st_recv, dn_send, dn_recv,
    far_send, far_recv, table_send, table_recv,
):
    f32, bf16 = jnp.float32, jnp.bfloat16
    MESH = pl.DeviceIdType.MESH
    me, me_e = lax.axis_index("dp"), lax.axis_index("expert")
    chips = n_dp // 2
    chip, core = me // 2, me % 2
    tiers = n_dp.bit_length() - 1
    half = n_dp // 2
    slots = ids.shape[1]
    pool_rows, width = tokens.shape
    hid = pre.shape[1] // 2
    rows_gu, rows_dn = gate_h.shape[1], down_h.shape[1]
    rows = (rows_gu, rows_gu, rows_dn)
    cols = (hid, hid, down_h.shape[2])
    lump = min(512, hid)
    peers_e = sorted(range(1, n_e), key=lambda d: -bin(d).count("1"))

    barrier = pltpu.get_barrier_semaphore()
    for d in range(1, n_e):
        pl.semaphore_signal(barrier, inc=1, device_id={"expert": me_e ^ d}, device_id_type=MESH)
    pl.semaphore_signal(barrier, inc=1, device_id={"dp": me ^ 1}, device_id_type=MESH)
    ends = (chip < chips - 1, chip >= 1)
    for way, there in zip((1, -1), ends):
        @pl.when(there)
        def _(way=way):
            pl.semaphore_signal(barrier, inc=1, device_id={"dp": me + 2 * way}, device_id_type=MESH)

    loads = [
        pltpu.make_async_copy(src, dst, in_sem.at[i])
        for i, (src, dst) in enumerate(
            (
                (gate_h.at[0], weights[GATE]), (up_h.at[0], weights[UP]), (down_h.at[0], weights[DOWN]),
                (tok_h, tokens), (cot_h, cot),
                (mom_gate_h.at[0], moments[GATE]), (mom_up_h.at[0], moments[UP]), (mom_down_h.at[0], moments[DOWN]),
            )
        )
    ]
    for copy in loads:
        copy.start()

    def remote(src, dst, ssem, rsem, device):
        return pltpu.make_async_remote_copy(
            src_ref=src, dst_ref=dst, send_sem=ssem, recv_sem=rsem, device_id=device, device_id_type=MESH
        )

    def block(index, size):
        return pl.ds(pl.multiple_of(index * size, size), size)

    def dot(a, b):
        return jnp.dot(a, b, preferred_element_type=f32)

    def dot_t(a, b):
        return lax.dot_general(a, b, (((1,), (1,)), ((), ())), preferred_element_type=f32)

    pending = []

    def send(*args):
        copy = remote(*args)
        copy.start()
        pending.append(copy)
        return copy

    mine_gu, mine_dn = block(me, rows_gu), block(me, rows_dn)
    loads[0].wait()
    gu_full[mine_gu, :hid] = weights[GATE][...].astype(bf16)
    loads[1].wait()
    gu_full[mine_gu, hid:] = weights[UP][...].astype(bf16)
    loads[2].wait()
    dn_full[mine_dn, :] = weights[DOWN][...].astype(bf16)

    pl.semaphore_wait(barrier, n_e + jnp.where(ends[0], 1, 0) + jnp.where(ends[1], 1, 0))

    id_copies = [None] + [
        send(ids, all_ids.at[d], id_send.at[d], id_recv.at[d], {"expert": me_e ^ d}) for d in range(1, n_e)
    ]
    all_ids[0] = ids[...]

    fulls, shard_rows = (gu_full, dn_full), (rows_gu, rows_dn)

    def shard(part, origin):
        return fulls[part].at[block(origin, shard_rows[part])]

    def along(way, hop, part):
        side = 0 if way > 0 else 1
        origin = me - 2 * way * hop
        return remote(
            shard(part, origin), shard(part, origin),
            line_send.at[side, hop, part], line_recv.at[side, hop, part], {"dp": me + 2 * way},
        )

    def arriving(way, hop, part):
        side = 0 if way > 0 else 1
        origin = me - 2 * way * (hop + 1)
        return remote(
            shard(part, origin), shard(part, origin),
            line_send.at[side, hop, part], line_recv.at[side, hop, part], {"dp": me ^ 1},
        )

    def across(way, hop, part):
        side = 0 if way > 0 else 1
        origin = me - 2 * way * hop
        return remote(
            shard(part, origin), shard(part, origin),
            pair_send.at[side, hop, part], pair_recv.at[side, hop, part], {"dp": me ^ 1},
        )

    def across_arriving(way, hop, part):
        side = 0 if way > 0 else 1
        origin = (me ^ 1) - 2 * way * hop
        return remote(
            shard(part, origin), shard(part, origin),
            pair_send.at[side, hop, part], pair_recv.at[side, hop, part], {"dp": me ^ 1},
        )

    def has(way, hop):
        behind = chip >= hop if way > 0 else chip < chips - hop
        ahead = chip < chips - 1 if way > 0 else chip >= 1
        return behind, ahead

    for part in (0, 1):
        for way in (1, -1):
            @pl.when(has(way, 0)[1])
            def _(way=way, part=part):
                along(way, 0, part).start()
    for part in (0, 1):
        across(1, 0, part).start()

    def forward(hop, part):
        for way in (1, -1):
            behind, ahead = has(way, hop + 1)

            @pl.when(behind)
            def _(way=way):
                arriving(way, hop, part).wait_recv()

            @pl.when(jnp.logical_and(behind, ahead))
            def _(way=way):
                along(way, hop + 1, part).start()

            @pl.when(behind)
            def _(way=way):
                across(way, hop + 1, part).start()

    def crossed(hop, part):
        if hop == 0:
            across_arriving(1, 0, part).wait_recv()
            return
        for way in (1, -1):
            @pl.when(has(way, hop)[0])
            def _(way=way):
                across_arriving(way, hop, part).wait_recv()

    lane = lax.broadcasted_iota(jnp.int32, (slots, 128), 1)

    def chosen(d, first=0, count=slots):
        column = jnp.transpose(jnp.broadcast_to(all_ids[d][:, first : first + count], (128, count)))
        return jnp.concatenate(
            [jnp.where(column == lane[:count] + c * 128, 1.0, 0.0).astype(bf16) for c in range(pool_rows // 128)],
            axis=1,
        )

    own_cols = block(me_e, width)
    pieces = ((0, slots // 4), (slots // 4, slots - slots // 4))

    def tokens_out(d, i):
        at = pl.ds(*pieces[i])
        stage_x[d - 1, at, :] = dot(chosen(d, *pieces[i]), tokens[...]).astype(bf16)
        send(
            stage_x.at[d - 1, at], routed.at[at, own_cols], tok_send.at[d, i], tok_recv.at[d, i], {"expert": me_e ^ d}
        )

    loads[3].wait()
    near = [d for d in range(1, n_e) if d & (d - 1) == 0]
    for i in (0, 1):
        for d in near:
            if i == 0:
                id_copies[d].wait_recv()
            tokens_out(d, i)
    for d in range(1, n_e):
        if d not in near:
            id_copies[d].wait_recv()
            tokens_out(d, 0)
            tokens_out(d, 1)
    loads[4].wait()
    for d in range(1, n_e):
        stage_c[d - 1] = dot(chosen(d), cot[...]).astype(bf16)
        send(stage_c.at[d - 1], cot_rows.at[:, own_cols], tok_send.at[d, 2], tok_recv.at[d, 2], {"expert": me_e ^ d})

    last_hop = chips - 1
    forward(0, 0)
    choice = chosen(0)
    routed[:, own_cols] = dot(choice, tokens[...]).astype(bf16)
    cot_rows[:, own_cols] = dot(choice, cot[...]).astype(bf16)
    forward(0, 1)

    route_column = jnp.transpose(jnp.broadcast_to(route[...], (128, slots)))

    def tokens_in(d, part):
        theirs, peer = block(me_e ^ d, width), {"expert": me_e ^ d}
        if part:
            remote(
                stage_c.at[d - 1], cot_rows.at[:, theirs], tok_send.at[d, 2], tok_recv.at[d, 2], peer
            ).wait_recv()
            return
        for i in (0, 1):
            at = pl.ds(*pieces[i])
            remote(
                stage_x.at[d - 1, at], routed.at[at, theirs], tok_send.at[d, i], tok_recv.at[d, i], peer
            ).wait_recv()

    def turn(d):
        e = me_e ^ d
        per = width // rows_gu
        flipped = jnp.transpose(routed[:, block(e, width)])
        for i in range(per):
            at = block(e * (per // 2) + i // 2, rows_gu)
            x_t[(i % 2) ^ core, at, :] = flipped[i * rows_gu : (i + 1) * rows_gu]

    def scale(d):
        for c in range(width // 128):
            at = pl.ds(pl.multiple_of((me_e ^ d) * width + c * 128, 128), 128)
            cot_rows[:, at] = (route_column * cot_rows[:, at].astype(f32)).astype(bf16)

    tall = min(256, slots)

    def multiply(origin, first):
        at = block(origin, 2 * rows_gu)
        for m in range(slots // tall):
            part = dot(routed[m * tall : (m + 1) * tall, at], gu_full[at, :])
            if first:
                pre[m * tall : (m + 1) * tall, :] = part
            else:
                pre[m * tall : (m + 1) * tall, :] += part

    def multiply_hop(hop):
        crossed(hop, 0)
        for way in (1, -1):
            @pl.when(has(way, hop)[0])
            def _(way=way):
                multiply(chip - way * hop, False)

    turn(0)
    scale(0)
    for d in range(1, n_e):
        tokens_in(d, 0)
        turn(d)
    crossed(0, 0)
    multiply(chip, True)
    for hop in range(1, chips):
        if hop == last_hop:
            tokens_in(1, 1)
            scale(1)
        if hop > 1:
            forward(hop - 1, 0)
        multiply_hop(hop)
        if 1 < hop < last_hop:
            forward(hop - 1, 1)

    step = 16

    def activate(i, carry):
        at = pl.ds(pl.multiple_of(i * step, step), step)
        gate_pre, up_pre = pre[at, :hid], pre[at, hid:]
        sig = jax.nn.sigmoid(gate_pre)
        act = gate_pre * sig
        hidden[at, :] = (act * up_pre).astype(bf16)
        pre[at, :hid] = up_pre * sig * (1.0 + gate_pre * (1.0 - sig))
        pre[at, hid:] = act
        return carry

    lax.fori_loop(0, slots // step, activate, 0, unroll=2)
    flipped = jnp.transpose(hidden[...])
    for p in range(n_dp):
        h_t[(p % 2) ^ core, (p // 2) * rows_dn : (p // 2 + 1) * rows_dn, :] = flipped[p * rows_dn : (p + 1) * rows_dn]

    offset = [(2 << t) - 2 - t for t in range(tiers)]
    flying, news, totals = {}, {}, {}

    def blocks_at(t):
        return n_dp >> (t + 1)

    def block_copy(m, t, k):
        size = blocks_at(t) // chunks_of(blocks_at(t)) * rows[m]
        at = pl.ds(k * size, size)
        src = sent[m] if t == 0 else outs[m][t - 1]
        return remote(
            src.at[at], ins[m][t].at[at], blk_send.at[m, t, k], blk_recv.at[m, t, k], {"dp": me ^ (1 << t)}
        )

    def launch_all(m, t, now=None):
        for k in range(chunks_of(blocks_at(t))):
            copy = block_copy(m, t, k)
            if now is None:
                copy.start()
            else:
                pl.when(now)(copy.start)
            if (m, t, k) not in flying:
                flying[m, t, k] = copy
                pending.append(copy)

    def gradient(m, away):
        total = half * rows[m]
        tile = min(256, total)
        parts = chunks_of(half)
        done = 0
        for i in range(total // tile):
            at = pl.ds(i * tile, tile)
            value = dot(x_t[1 if away else 0, at, :], both[:, m * hid : (m + 1) * hid]) * (1.0 / slots)
            if away:
                sent[m][at, :] = value.astype(bf16)
            else:
                own[m][at, :] = value
            while away and done < parts and (i + 1) * tile >= (done + 1) * (total // parts):
                flying[m, 0, done] = block_copy(m, 0, done)
                flying[m, 0, done].start()
                pending.append(flying[m, 0, done])
                done += 1

    down_copies = {}

    def down_away(d):
        at = block(me_e ^ d, width)
        sent[DOWN][:, at] = (dot(h_t[1], cot_rows[:, at]) * (1.0 / slots)).astype(bf16)
        down_copies[d] = send(
            sent[DOWN].at[:, at], ins[DOWN][0].at[:, at], dn_send.at[d], dn_recv.at[d], {"dp": me ^ 1}
        )

    def down_own(d):
        at = block(me_e ^ d, width)
        own[DOWN][:, at] = dot(h_t[0], cot_rows[:, at]) * (1.0 / slots)

    def low(t):
        return lax.shift_right_logical(me, 1) & ((1 << t) - 1)

    def bit_of(t):
        return lax.shift_right_logical(me, t) & 1

    def fold(x):
        return x[:8] + x[8:]

    def lanes(x):
        total = x[:, :128]
        for c in range(1, x.shape[1] // 128):
            total = total + x[:, c * 128 : (c + 1) * 128]
        return jnp.sum(total, axis=0, keepdims=True)

    def measure(m, t):
        blocks, steps = blocks_at(t), rows[m] // step
        parts = chunks_of(blocks)
        bit, base = bit_of(t), low(t)
        acc = tuple(jnp.zeros((8, lump), f32) for _ in range(3))

        def body(places, i, acc):
            j, r = i // steps, i % steps
            at_mine = pl.ds(pl.multiple_of(((j << t) + base) * rows[m] + r * step, step), step)
            at_other = pl.ds(pl.multiple_of(i * step, step), step)
            ab, aa, bb = acc
            for at in places:
                a = own[m][at_mine, at]
                b = ins[m][t][at_other, at].astype(f32)
                ab, aa, bb = ab + fold(a * b), aa + fold(a * a), bb + fold(b * b)
            return ab, aa, bb

        if m == DOWN and t == 0:
            for d in range(n_e):
                down_copies[d].wait_recv()
                first = (me_e ^ d) * width
                places = [pl.ds(pl.multiple_of(first + c, lump), lump) for c in range(0, width, lump)]
                acc = lax.fori_loop(0, blocks * steps, functools.partial(body, places), acc, unroll=2)
        else:
            per = blocks // parts * steps
            places = [pl.ds(c, lump) for c in range(0, cols[m], lump)]
            for k in range(parts):
                flying[m, t, k].wait_recv()
                acc = lax.fori_loop(
                    k * per, (k + 1) * per, functools.partial(body, places), acc, unroll=2 if per % 2 == 0 else 1
                )

        ab, aa, bb = (lanes(x) for x in acc)
        local = jnp.concatenate(
            [ab, jnp.where(bit == 0, aa, bb), jnp.where(bit == 0, bb, aa), jnp.zeros((5, 128), f32)], axis=0
        )
        stats[m, t] = local
        totals[m, t] = local
        news[m, t] = [
            send(
                stats.at[m, t], stats_in.at[m, offset[t] + d - 1],
                st_send.at[m, offset[t] + d - 1], st_recv.at[m, offset[t] + d - 1], {"dp": me ^ d},
            )
            for d in range((2 << t) - 1, 0, -1)
        ][::-1]

    def settle(m, t):
        total = totals[m, t]
        for d in range(1, 2 << t):
            news[m, t][d - 1].wait_recv()
            total = total + stats_in[m, offset[t] + d - 1]
        whole = jnp.sum(total, axis=1, keepdims=True)
        inner, bit = whole[0:1], bit_of(t)
        c_left, c_right = coefs(inner, whole[1:2]), coefs(inner, whole[2:3])
        c_mine = jnp.where(bit == 0, c_left, c_right)
        c_other = jnp.where(bit == 0, c_right, c_left)
        return jnp.broadcast_to(c_mine, (1, lump)), jnp.broadcast_to(c_other, (1, lump))

    def combine(m, t, c_m, c_o, count, which, store):
        steps, base = rows[m] // step, low(t)

        def body(i, carry):
            jj, r = i // steps, i % steps
            j = which(jj)
            at_mine = pl.ds(pl.multiple_of(((j << t) + base) * rows[m] + r * step, step), step)
            at_other = pl.ds(pl.multiple_of(j * rows[m] + r * step, step), step)
            for c in range(0, cols[m], lump):
                value = own[m][at_mine, c : c + lump] * c_m
                value = value + ins[m][t][at_other, c : c + lump].astype(f32) * c_o
                store(i, at_mine, pl.ds(c, lump), value)
            return carry

        n = count * steps
        lax.fori_loop(0, n, body, 0, unroll=2 if n % 2 == 0 else 1)

    def merge(m, t, then=None):
        c_m, c_o = settle(m, t)
        up = bit_of(t + 1)
        count = blocks_at(t + 1)

        def store_away(i, at, to, value):
            outs[m][t][pl.ds(pl.multiple_of(i * step, step), step), to] = value.astype(bf16)

        def store_own(i, at, to, value):
            own[m][at, to] = value

        combine(m, t, c_m, c_o, count, lambda j: 2 * j + 1 - up, store_away)
        if then is not None:
            then()
        combine(m, t, c_m, c_o, count, lambda j: 2 * j + up, store_own)

    new, following = (new_gate, new_up, new_down), (next_gate, next_up, next_down)

    def finish(m):
        t = tiers - 1
        c_m, c_o = settle(m, t)
        loads[5 + m].wait()

        def store(i, at, to, value):
            row = pl.ds(pl.multiple_of(i * step, step), step)
            update(m, row, to, value)

        combine(m, t, c_m, c_o, 1, lambda j: j, store)

    def update(m, row, to, value):
        momentum = momentum_decay * moments[m][row, to] + value
        following[m][0, row, to] = momentum
        new[m][0, row, to] = weights[m][row, to] - learning_rate * momentum

    same_way = bit_of(1) == bit_of(2)
    other_way = jnp.logical_not(same_way)

    far = {}

    def scatter(m):
        c_m, c_o = settle(m, 0)
        for r in (2, 3, 1):
            def store_far(i, at, to, value, r=r):
                far_out[pl.ds(pl.multiple_of((r - 1) * rows[m] + i * step, step), step), to] = value.astype(bf16)

            combine(m, 0, c_m, c_o, 1, lambda j, r=r: chip ^ r, store_far)
            at = pl.ds((r - 1) * rows[m], rows[m])
            far[r] = remote(far_out.at[at], far_in.at[at], far_send.at[r - 1], far_recv.at[r - 1], {"dp": me ^ (2 * r)})
            pending.append(far[r])
            if r == 3:
                pl.when(other_way)(far[2].start)
                far[3].start()

        def store_own(i, at, to, value):
            own[m][at, to] = value

        combine(m, 0, c_m, c_o, 1, lambda j: chip, store_own)

    def by_chip(swap, items):
        for b in (0, 1):
            bit = lax.shift_right_logical(chip, b) & 1
            items = {k: jnp.where(bit == 0, items[k], items[swap(k, 1 << b)]) for k in items}
        return items

    pairs4 = [(i, j) for i in range(4) for j in range(4)]

    def far_tiles(m, i, to):
        mine = pl.ds(pl.multiple_of(chip * rows[m] + i * step, step), step)
        tiles = [own[m][mine, to]]
        for r in (1, 2, 3):
            tiles.append(far_in[pl.ds(pl.multiple_of((r - 1) * rows[m] + i * step, step), step), to].astype(f32))
        return tiles

    def gram(m):
        for r in (1, 2, 3):
            far[r].wait_recv()
        wide = lump // 2
        upper = [(i, j) for i, j in pairs4 if i <= j]

        def body(i, acc):
            for c in range(0, cols[m], wide):
                v = far_tiles(m, i, pl.ds(c, wide))
                acc = tuple(x + fold(v[a] * v[b]) for x, (a, b) in zip(acc, upper))
            return acc

        acc = lax.fori_loop(0, rows[m] // step, body, tuple(jnp.zeros((8, wide), f32) for _ in upper))
        sums = {k: lanes(x) for k, x in zip(upper, acc)}
        sums = {(i, j): sums[min(i, j), max(i, j)] for i, j in pairs4}
        sums = by_chip(lambda k, s: (k[0] ^ s, k[1] ^ s), sums)
        local = jnp.concatenate([sums[k] for k in pairs4], axis=0)
        far_stats[...] = local
        totals[m, 1] = local
        news[m, 1] = [
            send(far_stats, far_stats_in.at[d - 1], table_send.at[d - 1], table_recv.at[d - 1], {"dp": me ^ d})
            for d in range(n_dp - 1, 0, -1)
        ][::-1]

    def finish_far(m):
        total = totals[m, 1]
        for d in range(1, n_dp):
            news[m, 1][d - 1].wait_recv()
            total = total + far_stats_in[d - 1]
        whole = jnp.sum(total, axis=1, keepdims=True)
        g = {(i, j): whole[4 * i + j : 4 * i + j + 1] for i, j in pairs4}
        share = {}
        for a, b in ((0, 1), (2, 3)):
            share[a], share[b] = coefs(g[a, b], g[a, a]), coefs(g[a, b], g[b, b])

        def norm(a, b):
            value = share[a] * share[a] * g[a, a] + 2.0 * share[a] * share[b] * g[a, b] + share[b] * share[b] * g[b, b]
            return jnp.maximum(value, 0.0)

        inner = sum(share[a] * share[b] * g[a, b] for a in (0, 1) for b in (2, 3))
        c_left, c_right = coefs(inner, norm(0, 1)), coefs(inner, norm(2, 3))
        w = {a: share[a] * (c_left if a < 2 else c_right) for a in range(4)}
        w = by_chip(lambda k, s: k ^ s, w)
        w = [jnp.broadcast_to(w[r], (1, lump)) for r in range(4)]
        loads[5 + m].wait()

        def body(i, carry):
            row = pl.ds(pl.multiple_of(i * step, step), step)
            for c in range(0, cols[m], lump):
                to = pl.ds(c, lump)
                v = far_tiles(m, i, to)
                update(m, row, to, v[0] * w[0] + v[1] * w[1] + (v[2] * w[2] + v[3] * w[3]))
            return carry

        lax.fori_loop(0, rows[m] // step, body, 0, unroll=2)

    down_away(0)
    for d in range(1, n_e):
        if d > 1:
            tokens_in(d, 1)
            scale(d)
        down_away(d)
    for d in range(n_e):
        down_own(d)
    forward(last_hop - 1, 1)
    measure(DOWN, 0)
    straight = chips == 4
    if straight:
        scatter(DOWN)
    else:
        merge(DOWN, 0)
        launch_all(DOWN, 1)

    for hop in range(chips):
        crossed(hop, 1)
    for m in range(slots // tall):
        at = slice(m * tall, (m + 1) * tall)
        back = dot_t(cot_rows[at, :], dn_full[...])
        both[at, :hid] = (back * pre[at, :hid]).astype(bf16)
        both[at, hid:] = (back * pre[at, hid:]).astype(bf16)

    def slot_back(d):
        weight = gu_full[block(me_e ^ d, width), :]
        value = dot_t(both[...], weight).astype(bf16)
        if d == 0:
            returned[0:slots, :] = value
            return None
        slot_grad[d - 1] = value
        return send(
            slot_grad.at[d - 1], returned.at[pl.ds(d * slots, slots)], ret_send.at[d], ret_recv.at[d],
            {"expert": me_e ^ d},
        )

    def pool_sum():
        for copy in back_copies:
            copy.wait_recv()
        tile = 256

        @pl.loop(0, pool_rows // tile)
        def _(t):
            at = pl.multiple_of(t * tile, tile)
            row = lax.broadcasted_iota(jnp.int32, (tile, slots), 0) + at
            pick = jnp.concatenate(
                [jnp.where(row == all_ids[d], 1.0, 0.0).astype(bf16) for d in range(n_e)], axis=1
            )
            pool[pl.ds(at, tile), :] = dot(pick, returned[...])

    gradient(GATE, True)
    gradient(GATE, False)
    gradient(UP, True)
    gradient(UP, False)
    measure(GATE, 0)

    def first_gate():
        if straight:
            launch_all(GATE, 1)
            pl.when(same_way)(far[2].start)

    merge(GATE, 0, first_gate)
    measure(UP, 0)
    back_copies = [slot_back(d) for d in peers_e]
    merge(UP, 0)
    slot_back(0)
    if straight:
        measure(GATE, 1)
        launch_all(UP, 1)
        merge(GATE, 1, lambda: launch_all(GATE, 2))
        measure(UP, 1)
        pl.when(other_way)(far[1].start)
        merge(UP, 1, lambda: launch_all(UP, 2))
        pl.when(same_way)(far[1].start)
        pool_sum()
        measure(GATE, 2)
        gram(DOWN)
        measure(UP, 2)
        finish(GATE)
        finish_far(DOWN)
        finish(UP)
    else:
        measure(DOWN, 1)
        launch_all(GATE, 1)
        merge(DOWN, 1)
        measure(GATE, 1)
        launch_all(DOWN, 2)
        launch_all(UP, 1)
        merge(GATE, 1)
        pool_sum()
        measure(UP, 1)
        launch_all(GATE, 2)
        merge(UP, 1)
        launch_all(UP, 2)
        for t in range(2, tiers):
            for m in (DOWN, GATE, UP):
                measure(m, t)
                if t == tiers - 1:
                    finish(m)
                else:
                    merge(m, t)
                    launch_all(m, t + 1)

    for part in (0, 1):
        across(1, 0, part).wait_send()
    for hop in range(chips):
        for part in (0, 1):
            for way in (1, -1):
                behind, ahead = has(way, hop)

                @pl.when(jnp.logical_and(behind, ahead))
                def _(way=way, hop=hop, part=part):
                    along(way, hop, part).wait_send()

                if hop:
                    @pl.when(behind)
                    def _(way=way, hop=hop, part=part):
                        across(way, hop, part).wait_send()
    for copy in pending:
        copy.wait_send()


def store_kernel(*refs):
    *pairs, sem = refs
    count = len(pairs) // 2
    copies = [pltpu.make_async_copy(pairs[i], pairs[count + i], sem.at[i]) for i in range(count)]
    for copy in copies:
        copy.start()
    for copy in copies:
        copy.wait()


def local(
    pool_tokens,
    pool_cotangent,
    token_ids,
    route_weights,
    gate_weight,
    up_weight,
    down_weight,
    momentum_gate,
    momentum_up,
    momentum_down,
):
    bf16, f32 = jnp.bfloat16, jnp.float32
    n_e, n_dp = lax.axis_size("expert"), lax.axis_size("dp")
    chips, half, tiers = n_dp // 2, n_dp // 2, n_dp.bit_length() - 1
    pool_rows, width = pool_tokens.shape
    slots = token_ids.shape[1]
    rows_gu, hid = gate_weight.shape[1:]
    rows_dn, full = down_weight.shape[1:]
    shapes = ((rows_gu, hid), (rows_gu, hid), (rows_dn, full))
    n_stats = sum((2 << t) - 1 for t in range(tiers))
    vmem, anywhere = pl.BlockSpec(memory_space=pltpu.VMEM), pl.BlockSpec(memory_space=pl.ANY)
    dma, buf = pltpu.SemaphoreType.DMA, pltpu.VMEM

    def per_matrix(blocks, kind):
        return [buf((blocks * r, c), kind) for r, c in shapes]

    def per_tier(first, kind):
        return [[buf(((n_dp >> (t + 1)) * r, c), kind) for t in range(first, tiers)] for r, c in shapes]

    like = [(x.shape, f32) for x in (gate_weight, up_weight, down_weight)]
    like = [*like, *like, ((pool_rows, width), f32)]
    results = pl.pallas_call(
        functools.partial(step_kernel, n_e, n_dp),
        out_shape=[buf(*x) for x in like],
        in_specs=[vmem] * 2 + [anywhere] * 8,
        out_specs=[vmem] * len(like),
        scratch_shapes=[
            buf((pool_rows, width), bf16),
            buf((pool_rows, width), bf16),
            per_matrix(1, f32),
            per_matrix(1, f32),
            buf((n_e, 1, slots), jnp.int32),
            buf((n_e - 1, slots, width), bf16),
            buf((n_e - 1, slots, width), bf16),
            buf((slots, full), bf16),
            buf((slots, full), bf16),
            buf((n_dp * rows_gu, 2 * hid), bf16),
            buf((n_dp * rows_dn, full), bf16),
            buf((2, half * rows_gu, slots), bf16),
            buf((2, half * rows_dn, slots), bf16),
            buf((slots, hid), bf16),
            buf((slots, 2 * hid), f32),
            buf((slots, 2 * hid), bf16),
            buf((n_e - 1, slots, width), bf16),
            buf((n_e * slots, width), bf16),
            per_matrix(half, f32),
            per_matrix(half, bf16),
            per_tier(1, bf16),
            per_tier(0, bf16),
            buf((3, tiers, 8, 128), f32),
            buf((3, n_stats, 8, 128), f32),
            buf((3 * rows_dn, full), bf16),
            buf((3 * rows_dn, full), bf16),
            buf((16, 128), f32),
            buf((7, 16, 128), f32),
            dma((8,)), dma((n_e,)), dma((n_e,)), dma((n_e, 3)), dma((n_e, 3)),
            dma((2, chips, 2)), dma((2, chips, 2)), dma((2, chips, 2)), dma((2, chips, 2)),
            dma((n_e,)), dma((n_e,)), dma((3, tiers, 2)), dma((3, tiers, 2)), dma((3, n_stats)), dma((3, n_stats)), dma((n_e,)), dma((n_e,)),
            dma((3,)), dma((3,)), dma((7,)), dma((7,)),
        ],
        compiler_params=pltpu.CompilerParams(
            collective_id=1, has_side_effects=True, vmem_limit_bytes=54 * 1024 * 1024
        ),
    )(
        token_ids, route_weights, pool_tokens, pool_cotangent, gate_weight, up_weight, down_weight,
        momentum_gate, momentum_up, momentum_down,
    )
    return pl.pallas_call(
        store_kernel,
        out_shape=[jax.ShapeDtypeStruct(*x) for x in like],
        in_specs=[vmem] * len(like),
        out_specs=[anywhere] * len(like),
        scratch_shapes=[dma((len(like),))],
        compiler_params=pltpu.CompilerParams(vmem_limit_bytes=1024 * 1024),
    )(*results)


def solution(mesh):
    in_specs = (
        P("dp", "expert"),
        P("dp", "expert"),
        P("expert", "dp"),
        P("expert", "dp"),
        P("expert", "dp", None),
        P("expert", "dp", None),
        P("expert", "dp", None),
        P("expert", "dp", None),
        P("expert", "dp", None),
        P("expert", "dp", None),
    )
    out_specs = (
        P("expert", "dp", None),
        P("expert", "dp", None),
        P("expert", "dp", None),
        P("expert", "dp", None),
        P("expert", "dp", None),
        P("expert", "dp", None),
        P("dp", "expert"),
    )
    return jax.shard_map(local, mesh=mesh, in_specs=in_specs, out_specs=out_specs, check_vma=False)
```
